128 devices in a mesh: north: 32 (over y, x, core), deep: 4 (over z).
Axes of the slice: x: 4, y: 4, z: 4, core: 2. Of those that a mesh axis runs over, the one named last changes fastest.
Arguments:
- velocity: float32 [4, 512, 256, 256], P(None, None, 'north', 'deep'), may hold values from -6 to 6
- coupling: float32 [4, 4], replicated, may hold values from -4 to 4
- symbol_x: float32 [512], replicated, may hold values from 0.3 to 3
- symbol_y: float32 [256], replicated, may hold values from 0.3 to 3
- symbol_z: float32 [256], replicated, may hold values from 0.3 to 3
Outputs:
- spectrum: float32 [4, 512, 256, 256], P(None, 'north', 'deep')
The draws below stay inside these ranges and needn't reach their ends.
All inputs are finite; a program needn't handle non-finite values.
Results may differ from the reference program's by a relative error of at most 0.00007.
Values sent between devices are 32-bit elements; how exact they have to be, the bound alone decides.
A program may use at most 128 MiB of HBM per device.

```python
import jax
import jax.numpy as jnp
from jax import lax

GRID_X = 512
GRID_Y = 256
GRID_Z = 256
FIELDS = 4


def steps_of(rng, dims, pieces, least, top_value):
    loudness = 1.0
    for position, shards_of in pieces:
        steps = jax.random.uniform(jax.random.fold_in(jax.random.fold_in(rng, 6), position), (shards_of,), jnp.float32, least / len(pieces), top_value / len(pieces))
        loudness = loudness * jnp.repeat(jnp.exp(steps), dims[position] // shards_of).reshape((-1,) + (1,) * (len(dims) - 1 - position))
    return loudness


def normal_values(key, shape, deviation, limit, pieces=(), kind=jnp.bfloat16):
    array = jax.random.normal(key, shape, jnp.float32) * deviation
    if len(pieces) > 0:
        array = steps_of(key, shape, pieces, -0.22, 0.18) * array
    return jnp.clip(array, min=-limit, max=limit).astype(kind)


def setup_inputs(seed: int = 0) -> dict:
    key_list = jax.random.split(jax.random.key(seed), 6)
    velocity = normal_values(key_list[0], (FIELDS, GRID_X, GRID_Y, GRID_Z), 1.0, 6.0, ((2, 32), (3, 4)), jnp.float32)
    coupling = normal_values(key_list[1], (FIELDS, FIELDS), 0.7, 4.0, (), jnp.float32)
    symbol_x = jnp.clip(jax.random.uniform(key_list[2], (GRID_X,), jnp.float32, 0.3, 3.0), 0.3, 3.0)
    symbol_y = jnp.clip(jax.random.uniform(key_list[3], (GRID_Y,), jnp.float32, 0.3, 3.0), 0.3, 3.0)
    symbol_z = jnp.clip(jax.random.uniform(key_list[4], (GRID_Z,), jnp.float32, 0.3, 3.0), 0.3, 3.0)
    return dict(velocity=velocity, coupling=coupling, symbol_x=symbol_x, symbol_y=symbol_y, symbol_z=symbol_z)


def basis_table(count):
    rank = jnp.arange(count)
    angle = (jnp.pi / (count + 1)) * (((rank[:, None] + 1) * (rank[None, :] + 1)) % (2 * count + 2)).astype(jnp.float32)
    return jnp.sin(angle) * (2.0 / (count + 1)) ** 0.5


def along_dim(values, dim):
    moved = jnp.tensordot(values, basis_table(values.shape[dim]), axes=([dim], [0]), precision=lax.Precision.HIGHEST)
    return jnp.moveaxis(moved, -1, dim)


def reference(velocity, coupling, symbol_x, symbol_y, symbol_z):
    spectrum = velocity
    spectrum = along_dim(spectrum, 1)
    spectrum = along_dim(spectrum, 2)
    spectrum = along_dim(spectrum, 3)
    symbol = symbol_x[:, None, None] + symbol_y[None, :, None] + symbol_z[None, None, :]
    weight_xyz = 1.0 / (1.0 + symbol)
    mixed_fields = jnp.einsum("ab,bxyz->axyz", coupling, spectrum, precision=lax.Precision.HIGHEST)
    spectrum = weight_xyz * spectrum + (1.0 - weight_xyz) * mixed_fields
    return spectrum
```

```python
import functools

import jax
import jax.numpy as jnp
import numpy as np
from jax import lax
from jax.experimental import pallas as pl
from jax.experimental.pallas import tpu as pltpu
from jax.sharding import PartitionSpec as P

MESH = pl.DeviceIdType.MESH
F32, BF16 = jnp.float32, jnp.bfloat16
CHUNKS = 8
GROUPS = ((0, 1), (1, 3), (3, 8))


def basis_table(count):
    rank = np.arange(1, count + 1)
    turns = (rank[:, None] * rank[None, :]) % (2 * count + 2)
    return np.sin(np.pi * turns / (count + 1)) * np.sqrt(2.0 / (count + 1))


def two_parts(table):
    high = table.astype(BF16)
    low = (table - high.astype(np.float64)).astype(BF16)
    return np.stack([high, low])


def split(values):
    high = values.astype(BF16)
    return high, (values - high.astype(F32)).astype(BF16)


def dot(a, b, transposed=False):
    dims = (((1,), (1 if transposed else 0,)), ((), ()))
    return lax.dot_general(a, b, dims, preferred_element_type=F32)


def product(a_high, a_low, b_high, b_low, transposed=False):
    small = dot(a_high, b_low, transposed) + dot(a_low, b_high, transposed)
    return dot(a_high, b_high, transposed) + small


def kernel(
    nn, nd, v_hbm, hx_hbm, hy_hbm, coupling, sym_x, sym_y, sym_z, out_hbm,
    vbuf, vhi, vlo, hx, hy, sbuf, rbuf, dsend, drecv, obuf, syz,
    vsem, hsem, ssem, rsem, dssem, drsem, osem,
):
    fields, ny, nz, nx = v_hbm.shape
    chunks = sbuf.shape[0]
    share_x = nx // nn
    rows = share_x // chunks
    wide = fields * nz
    tiles = wide // 128
    full_y = nn * ny
    share_y = full_y // nd
    piece = rows * tiles * ny
    me, deep = lax.axis_index("north"), lax.axis_index("deep")

    def north_peer(i):
        my, mx, mc = me // 8, (me // 2) % 4, me % 2
        return ((my + i // 8) % 4) * 8 + ((mx + (i // 2) % 4) % 4) * 2 + (mc + i % 2) % 2

    def load_v(y):
        return pltpu.make_async_copy(v_hbm.at[:, y], vbuf.at[y], vsem.at[y])

    load_hx = pltpu.make_async_copy(hx_hbm, hx, hsem.at[0])
    load_hy = pltpu.make_async_copy(hy_hbm, hy, hsem.at[1])
    load_hx.start()
    for y in range(ny):
        load_v(y).start()
    load_hy.start()

    barrier = pltpu.get_barrier_semaphore()

    @pl.loop(1, nn)
    def _(i):
        pl.semaphore_signal(
            barrier, inc=1, device_id={"north": north_peer(i), "deep": deep}, device_id_type=MESH
        )

    for i in range(1, nd):
        pl.semaphore_signal(
            barrier, inc=1, device_id={"north": me, "deep": (deep + i) % nd}, device_id_type=MESH
        )

    lane = lax.broadcasted_iota(jnp.int32, (share_y, full_y), 1)
    row = lax.broadcasted_iota(jnp.int32, (share_y, full_y), 0)
    mine = jnp.where(lane == row + deep * share_y, sym_y[...], 0.0)
    syz[...] = jnp.sum(mine, axis=1, keepdims=True) + sym_z[...]

    def transform_x(y, first, last):
        span = nn * rows
        pick = pl.ds(first * span, (last - first) * span)
        result = product(
            hx[0, pick, :], hx[1, pick, :], vhi[y], vlo[y], transposed=True
        )
        for c in range(first, last):
            part = result[(c - first) * span : (c - first + 1) * span]
            for t in range(tiles):
                sbuf[c, pl.ds(t * ny + y, span, stride=tiles * ny), :] = part[:, t * 128 : (t + 1) * 128]

    def send_north(c):
        @pl.loop(1, nn)
        def _(i):
            peer = north_peer(i)
            pltpu.make_async_remote_copy(
                src_ref=sbuf.at[c, pl.ds(pl.multiple_of(peer * piece, piece), piece)],
                dst_ref=rbuf.at[c, me],
                send_sem=ssem.at[c],
                recv_sem=rsem.at[c],
                device_id={"north": peer, "deep": deep},
                device_id_type=MESH,
            ).start()

        rbuf[c, me] = sbuf[c, pl.ds(pl.multiple_of(me * piece, piece), piece), :]

    def all_north(c):
        return pltpu.make_async_remote_copy(
            src_ref=rbuf.at[c, pl.ds(0, nn - 1)],
            dst_ref=rbuf.at[c, pl.ds(0, nn - 1)],
            send_sem=ssem.at[c],
            recv_sem=rsem.at[c],
            device_id={"north": me, "deep": deep},
            device_id_type=MESH,
        )

    def all_deep(c):
        return pltpu.make_async_remote_copy(
            src_ref=drecv.at[c, pl.ds(0, nd - 1)],
            dst_ref=drecv.at[c, pl.ds(0, nd - 1)],
            send_sem=dssem.at[c],
            recv_sem=drsem.at[c],
            device_id={"north": me, "deep": deep},
            device_id_type=MESH,
        )

    load_hx.wait()
    for y in range(ny):
        load_v(y).wait()
        high, low = split(vbuf[y].reshape(wide, nx))
        vhi[y] = high
        vlo[y] = low
        transform_x(y, *GROUPS[0])
    pl.semaphore_wait(barrier, nn - 1 + nd - 1)
    for first, last in GROUPS:
        if first > 0:
            @pl.loop(0, ny)
            def _(y):
                transform_x(y, first, last)

        for c in range(first, last):
            send_north(c)
    load_hy.wait()

    def stage_y(c):
        all_north(c).wait_recv()
        for j in range(rows):
            columns = [
                rbuf[c, :, pl.ds((j * tiles + t) * ny, ny), :].reshape(full_y, 128) for t in range(tiles)
            ]
            high, low = split(jnp.concatenate(columns, axis=1))
            result = product(hy[0], hy[1], high, low)
            for d in range(nd):
                dsend[c, d, j] = result[d * share_y : (d + 1) * share_y]
        for i in range(1, nd):
            peer = (deep + i) % nd
            pltpu.make_async_remote_copy(
                src_ref=dsend.at[c, peer],
                dst_ref=drecv.at[c, deep],
                send_sem=dssem.at[c],
                recv_sem=drsem.at[c],
                device_id={"north": me, "deep": peer},
                device_id_type=MESH,
            ).start()
        drecv[c, deep] = dsend[c, deep]

    lower = lax.broadcasted_iota(jnp.int32, (share_y, 128), 1) < nz

    def copy_out(c):
        return pltpu.make_async_copy(
            obuf.at[:, pl.ds(c * rows, rows)], out_hbm.at[:, pl.ds(c * rows, rows)], osem.at[c]
        )

    def stage_z(c):
        all_deep(c).wait_recv()
        for j in range(rows):
            lines = []
            for t in range(tiles):
                parts = [drecv[c, d, j, :, t * 128 : (t + 1) * 128] for d in range(nd)]
                turned = [pltpu.roll(p, nz, 1) for p in parts]
                even = [jnp.where(lower, parts[d], turned[d + 1]) for d in range(0, nd, 2)]
                odd = [jnp.where(lower, turned[d], parts[d + 1]) for d in range(0, nd, 2)]
                lines.append(jnp.concatenate(even, axis=1))
                lines.append(jnp.concatenate(odd, axis=1))
            high, low = split(jnp.concatenate(lines, axis=0))
            result = product(high, low, hy[0], hy[1])
            old = [result[f * share_y : (f + 1) * share_y] for f in range(fields)]
            x = c * rows + j
            weight = 1.0 / (1.0 + (sym_x[me * share_x + x] + syz[...]))
            rest = 1.0 - weight
            for a in range(fields):
                mixed = coupling[a, 0] * old[0]
                for b in range(1, fields):
                    mixed = mixed + coupling[a, b] * old[b]
                obuf[a, x] = weight * old[a] + rest * mixed
        copy_out(c).start()

    stage_y(0)

    @pl.loop(1, chunks)
    def _(c):
        stage_y(c)
        stage_z(c - 1)

    stage_z(chunks - 1)

    @pl.loop(0, chunks)
    def _(c):
        all_north(c).wait_send()
        all_deep(c).wait_send()
        copy_out(c).wait()


def on_device(nn, nd, velocity, coupling, symbol_x, symbol_y, symbol_z):
    fields, nx, ny, nz = velocity.shape
    share_x = nx // nn
    rows = share_x // CHUNKS
    full_y, full_z = ny * nn, nz * nd
    share_y = full_y // nd
    wide = fields * nz
    tiles = wide // 128
    order = np.arange(nx).reshape(nn, CHUNKS, rows).transpose(1, 0, 2).reshape(-1)
    table_x = jnp.asarray(two_parts(basis_table(nx)[order]))
    table_y = jnp.asarray(two_parts(basis_table(full_y)))
    anywhere = pl.BlockSpec(memory_space=pl.ANY)
    scalars = pl.BlockSpec(memory_space=pltpu.SMEM)
    vector = pl.BlockSpec(memory_space=pltpu.VMEM)
    dma = pltpu.SemaphoreType.DMA
    return pl.pallas_call(
        functools.partial(kernel, nn, nd),
        out_shape=jax.ShapeDtypeStruct((fields, share_x, share_y, full_z), F32),
        in_specs=[anywhere, anywhere, anywhere, scalars, scalars, vector, vector],
        out_specs=anywhere,
        scratch_shapes=[
            pltpu.VMEM((ny, fields, nz, nx), F32),
            pltpu.VMEM((ny, wide, nx), BF16),
            pltpu.VMEM((ny, wide, nx), BF16),
            pltpu.VMEM((2, nx, nx), BF16),
            pltpu.VMEM((2, full_y, full_y), BF16),
            pltpu.VMEM((CHUNKS, nn * rows * tiles * ny, 128), F32),
            pltpu.VMEM((CHUNKS, nn, rows * tiles * ny, 128), F32),
            pltpu.VMEM((CHUNKS, nd, rows, share_y, wide), F32),
            pltpu.VMEM((CHUNKS, nd, rows, share_y, wide), F32),
            pltpu.VMEM((fields, share_x, share_y, full_z), F32),
            pltpu.VMEM((share_y, full_z), F32),
            dma((ny,)), dma((2,)),
            dma((CHUNKS,)), dma((CHUNKS,)), dma((CHUNKS,)), dma((CHUNKS,)), dma((CHUNKS,)),
        ],
        compiler_params=pltpu.CompilerParams(
            collective_id=0, has_side_effects=True, vmem_limit_bytes=56 << 20
        ),
    )(
        jnp.transpose(velocity, (0, 2, 3, 1)), table_x, table_y, coupling, symbol_x,
        symbol_y.reshape(1, full_y), symbol_z.reshape(1, full_z),
    )


def solution(mesh):
    placed = (P(None, None, "north", "deep"), P(), P(), P(), P())
    return jax.shard_map(
        functools.partial(on_device, mesh.shape["north"], mesh.shape["deep"]),
        mesh=mesh,
        in_specs=placed,
        out_specs=P(None, "north", "deep", None),
        check_vma=False,
    )
```

```python
import functools

import jax
import jax.numpy as jnp
import numpy as np
from jax import lax
from jax.experimental import pallas as pl
from jax.experimental.pallas import tpu as pltpu
from jax.sharding import PartitionSpec as P

MESH = pl.DeviceIdType.MESH
F32, BF16 = jnp.float32, jnp.bfloat16
CHUNKS = 16
GROUPS = ((0, 2), (2, 8), (8, 16))


def basis_table(count):
    rank = np.arange(1, count + 1)
    turns = (rank[:, None] * rank[None, :]) % (2 * count + 2)
    return np.sin(np.pi * turns / (count + 1)) * np.sqrt(2.0 / (count + 1))


def two_parts(table):
    high = table.astype(BF16)
    low = (table - high.astype(np.float64)).astype(BF16)
    return np.stack([high, low])


def split(values):
    high = values.astype(BF16)
    return high, (values - high.astype(F32)).astype(BF16)


def dot(a, b, transposed=False):
    dims = (((1,), (1 if transposed else 0,)), ((), ()))
    return lax.dot_general(a, b, dims, preferred_element_type=F32)


def product(a_high, a_low, b_high, b_low, transposed=False):
    count = a_high.shape[0]
    both = dot(jnp.concatenate([a_high, a_low], axis=0), b_high, transposed)
    return both[:count] + (both[count:] + dot(a_high, b_low, transposed))


def kernel(
    nn, nd, v_hbm, hx_hbm, hy_hbm, coupling_hbm, sym_x_hbm, sym_y_hbm, sym_z_hbm, out,
    vbuf, vhi, vlo, hx, hy, sbuf, rbuf, dsend, drecv, syz, coupling, sym_x, sym_y, sym_z,
    vsem, hsem, ssem, rsem, dssem, drsem,
):
    fields, ny, nz, nx = v_hbm.shape
    chunks = sbuf.shape[0]
    share_x = nx // nn
    rows = share_x // chunks
    wide = fields * nz
    tiles = wide // 128
    full_y = nn * ny
    share_y = full_y // nd
    piece = rows * tiles * ny
    me, deep = lax.axis_index("north"), lax.axis_index("deep")

    loads = [
        pltpu.make_async_copy(a, b, hsem.at[k])
        for k, (a, b) in enumerate((
            (hx_hbm, hx), (hy_hbm, hy), (coupling_hbm, coupling), (sym_x_hbm, sym_x),
            (sym_y_hbm, sym_y), (sym_z_hbm, sym_z),
        ))
    ]
    load_v = [pltpu.make_async_copy(v_hbm.at[:, y], vbuf.at[y], vsem.at[y]) for y in range(ny)]
    loads[0].start()
    for copy in load_v:
        copy.start()
    for copy in loads[1:]:
        copy.start()

    along_y = [lax.rem(me // 8 + i, 4) * 8 for i in range(4)]
    along_x = [lax.rem(me // 2 + i, 4) * 2 for i in range(4)]
    cores = [lax.rem(me + i, 2) for i in range(2)]
    steps = [(a, b, c) for a in range(4) for b in range(4) for c in range(2)][1:]
    others = [along_y[a] + along_x[b] + cores[c] for a, b, c in steps]
    above = [lax.rem(deep + i, nd) for i in range(1, nd)]

    barrier = pltpu.get_barrier_semaphore()
    for peer in others:
        pl.semaphore_signal(
            barrier, inc=1, device_id={"north": peer, "deep": deep}, device_id_type=MESH
        )
    for peer in above:
        pl.semaphore_signal(
            barrier, inc=1, device_id={"north": me, "deep": peer}, device_id_type=MESH
        )

    def transform_x(y, first, last, high, low):
        span = nn * rows
        pick = pl.ds(first * span, (last - first) * span)
        result = product(hx[0, pick, :], hx[1, pick, :], high, low, transposed=True)
        for c in range(first, last):
            part = result[(c - first) * span : (c - first + 1) * span]
            for t in range(tiles):
                sbuf[c, pl.ds(t * ny + y, span, stride=tiles * ny), :] = part[:, t * 128 : (t + 1) * 128]

    def send_north(c):
        for peer in others:
            pltpu.make_async_remote_copy(
                src_ref=sbuf.at[c, pl.ds(pl.multiple_of(peer * piece, piece), piece)],
                dst_ref=rbuf.at[c, me],
                send_sem=ssem.at[c],
                recv_sem=rsem.at[c],
                device_id={"north": peer, "deep": deep},
                device_id_type=MESH,
            ).start()
        rbuf[c, me] = sbuf[c, pl.ds(pl.multiple_of(me * piece, piece), piece), :]

    def all_north(c):
        return pltpu.make_async_remote_copy(
            src_ref=rbuf.at[c, pl.ds(0, nn - 1)],
            dst_ref=rbuf.at[c, pl.ds(0, nn - 1)],
            send_sem=ssem.at[c],
            recv_sem=rsem.at[c],
            device_id={"north": me, "deep": deep},
            device_id_type=MESH,
        )

    def all_deep(c):
        return pltpu.make_async_remote_copy(
            src_ref=drecv.at[c, pl.ds(0, nd - 1)],
            dst_ref=drecv.at[c, pl.ds(0, nd - 1)],
            send_sem=dssem.at[c],
            recv_sem=drsem.at[c],
            device_id={"north": me, "deep": deep},
            device_id_type=MESH,
        )

    def group_x(first, last):
        @pl.loop(0, ny)
        def _(y):
            transform_x(y, first, last, vhi[y], vlo[y])

        @pl.loop(first, last)
        def _(c):
            send_north(c)

    def stage_y(c):
        all_north(c).wait_recv()
        for j in range(rows):
            columns = [
                rbuf[c, :, pl.ds((j * tiles + t) * ny, ny), :].reshape(full_y, 128) for t in range(tiles)
            ]
            high, low = split(jnp.concatenate(columns, axis=1))
            result = product(hy[0], hy[1], high, low)
            for d in range(nd):
                dsend[c, d, j] = result[d * share_y : (d + 1) * share_y]
        for peer in above:
            pltpu.make_async_remote_copy(
                src_ref=dsend.at[c, peer],
                dst_ref=drecv.at[c, deep],
                send_sem=dssem.at[c],
                recv_sem=drsem.at[c],
                device_id={"north": me, "deep": peer},
                device_id_type=MESH,
            ).start()
        drecv[c, deep] = dsend[c, deep]

    lower = lax.broadcasted_iota(jnp.int32, (share_y, 128), 1) < nz

    def stage_z(c):
        all_deep(c).wait_recv()
        for j in range(rows):
            lines = []
            for t in range(tiles):
                parts = [drecv[c, d, j, :, t * 128 : (t + 1) * 128] for d in range(nd)]
                turned = [pltpu.roll(p, nz, 1) for p in parts]
                even = [jnp.where(lower, parts[d], turned[d + 1]) for d in range(0, nd, 2)]
                odd = [jnp.where(lower, turned[d], parts[d + 1]) for d in range(0, nd, 2)]
                lines.append(jnp.concatenate(even, axis=1))
                lines.append(jnp.concatenate(odd, axis=1))
            high, low = split(jnp.concatenate(lines, axis=0))
            result = product(high, low, hy[0], hy[1])
            old = [result[f * share_y : (f + 1) * share_y] for f in range(fields)]
            x = c * rows + j
            weight = 1.0 / (1.0 + (sym_x[me * share_x + x] + syz[...]))
            rest = 1.0 - weight
            for a in range(fields):
                mixed = coupling[a, 0] * old[0]
                for b in range(1, fields):
                    mixed = mixed + coupling[a, b] * old[b]
                out[a, x] = weight * old[a] + rest * mixed

    loads[0].wait()
    for copy in load_v:
        copy.wait()
    for y in range(ny):
        high, low = split(vbuf[y].reshape(wide, nx))
        vhi[y] = high
        vlo[y] = low
        transform_x(y, *GROUPS[0], high, low)
    pl.semaphore_wait(barrier, nn - 1 + nd - 1)

    @pl.loop(*GROUPS[0])
    def _(c):
        send_north(c)

    group_x(*GROUPS[1])
    for copy in loads[1:]:
        copy.wait()
    stage_y(0)
    group_x(*GROUPS[2])

    lane = lax.broadcasted_iota(jnp.int32, (share_y, full_y), 1)
    row = lax.broadcasted_iota(jnp.int32, (share_y, full_y), 0)
    mine = jnp.where(lane == row + deep * share_y, sym_y[...], 0.0)
    syz[...] = jnp.sum(mine, axis=1, keepdims=True) + sym_z[...]

    @pl.loop(1, chunks)
    def _(c):
        stage_y(c)
        stage_z(c - 1)

    stage_z(chunks - 1)

    @pl.loop(0, chunks)
    def _(c):
        all_north(c).wait_send()
        all_deep(c).wait_send()


def on_device(nn, nd, velocity, coupling, symbol_x, symbol_y, symbol_z):
    fields, nx, ny, nz = velocity.shape
    share_x = nx // nn
    rows = share_x // CHUNKS
    full_y, full_z = ny * nn, nz * nd
    share_y = full_y // nd
    wide = fields * nz
    tiles = wide // 128
    order = np.arange(nx).reshape(nn, CHUNKS, rows).transpose(1, 0, 2).reshape(-1)
    table_x = jnp.asarray(two_parts(basis_table(nx)[order]))
    table_y = jnp.asarray(two_parts(basis_table(full_y)))
    dma = pltpu.SemaphoreType.DMA
    return pl.pallas_call(
        functools.partial(kernel, nn, nd),
        out_shape=jax.ShapeDtypeStruct((fields, share_x, share_y, full_z), F32),
        in_specs=[pl.BlockSpec(memory_space=pltpu.MemorySpace.HBM)] * 7,
        out_specs=pl.BlockSpec(memory_space=pltpu.VMEM),
        scratch_shapes=[
            pltpu.VMEM((ny, fields, nz, nx), F32),
            pltpu.VMEM((ny, wide, nx), BF16),
            pltpu.VMEM((ny, wide, nx), BF16),
            pltpu.VMEM((2, nx, nx), BF16),
            pltpu.VMEM((2, full_y, full_y), BF16),
            pltpu.VMEM((CHUNKS, nn * rows * tiles * ny, 128), F32),
            pltpu.VMEM((CHUNKS, nn, rows * tiles * ny, 128), F32),
            pltpu.VMEM((CHUNKS, nd, rows, share_y, wide), F32),
            pltpu.VMEM((CHUNKS, nd, rows, share_y, wide), F32),
            pltpu.VMEM((share_y, full_z), F32),
            pltpu.SMEM((fields, fields), F32),
            pltpu.SMEM((nx,), F32),
            pltpu.VMEM((1, full_y), F32),
            pltpu.VMEM((1, full_z), F32),
            dma((ny,)), dma((6,)),
            dma((CHUNKS,)), dma((CHUNKS,)), dma((CHUNKS,)), dma((CHUNKS,)),
        ],
        compiler_params=pltpu.CompilerParams(
            collective_id=0, has_side_effects=True, vmem_limit_bytes=32 << 20
        ),
    )(*(
        pltpu.with_memory_space_constraint(array, pltpu.MemorySpace.HBM)
        for array in (
            jnp.transpose(velocity, (0, 2, 3, 1)), table_x, table_y, coupling, symbol_x,
            symbol_y.reshape(1, full_y), symbol_z.reshape(1, full_z),
        )
    ))


def solution(mesh):
    placed = (P(None, None, "north", "deep"), P(), P(), P(), P())
    return jax.shard_map(
        functools.partial(on_device, mesh.shape["north"], mesh.shape["deep"]),
        mesh=mesh,
        in_specs=placed,
        out_specs=P(None, "north", "deep", None),
        check_vma=False,
    )
```

```python
import functools

import jax
import jax.numpy as jnp
import numpy as np
from jax import lax
from jax.experimental import pallas as pl
from jax.experimental.pallas import tpu as pltpu
from jax.sharding import PartitionSpec as P

MESH = pl.DeviceIdType.MESH
F32, BF16 = jnp.float32, jnp.bfloat16
CHUNKS = 16
FIRST = 2
PLAN = ((2, 8), "start", (8, 11), 1, (11, 14), 2, (14, 16))
LAG = 4


def basis_table(count):
    rank = np.arange(1, count + 1)
    turns = (rank[:, None] * rank[None, :]) % (2 * count + 2)
    return np.sin(np.pi * turns / (count + 1)) * np.sqrt(2.0 / (count + 1))


def two_parts(table):
    high = table.astype(BF16)
    low = (table - high.astype(np.float64)).astype(BF16)
    return np.stack([high, low])


def split(values):
    high = values.astype(BF16)
    return high, (values - high.astype(F32)).astype(BF16)


def dot(a, b, transposed=False):
    dims = (((1,), (1 if transposed else 0,)), ((), ()))
    return lax.dot_general(a, b, dims, preferred_element_type=F32)


def product(a_high, a_low, b_high, b_low, transposed=False):
    count = a_high.shape[0]
    both = dot(jnp.concatenate([a_high, a_low], axis=0), b_high, transposed)
    return both[:count] + (both[count:] + dot(a_high, b_low, transposed))


def kernel(
    nn, nd, v_hbm, hx_hbm, hy_hbm, coupling_hbm, sym_x_hbm, sym_y_hbm, sym_z_hbm, out,
    vbuf, vhi, vlo, hx, hy, sbuf, rbuf, dsend, drecv, syz, coupling, sym_x, sym_y, sym_z,
    vsem, hsem, ssem, rsem, dssem, drsem,
):
    fields, ny, nz, nx = v_hbm.shape
    chunks = sbuf.shape[0]
    share_x = nx // nn
    rows = share_x // chunks
    wide = fields * nz
    tiles = wide // 128
    full_y = nn * ny
    share_y = full_y // nd
    piece = rows * ny
    me, deep = lax.axis_index("north"), lax.axis_index("deep")

    loads = [
        pltpu.make_async_copy(a, b, hsem.at[k])
        for k, (a, b) in enumerate((
            (hx_hbm, hx), (hy_hbm, hy), (coupling_hbm, coupling), (sym_x_hbm, sym_x),
            (sym_y_hbm, sym_y), (sym_z_hbm, sym_z),
        ))
    ]
    load_v = [pltpu.make_async_copy(v_hbm.at[:, y], vbuf.at[y], vsem.at[y]) for y in range(ny)]
    loads[0].start()
    for copy in load_v:
        copy.start()

    along_y = [lax.rem(me // 8 + i, 4) * 8 for i in range(4)]
    along_x = [lax.rem(me // 2 + i, 4) * 2 for i in range(4)]
    cores = [lax.rem(me + i, 2) for i in range(2)]
    steps = [(a, b, c) for a in range(4) for b in range(4) for c in range(2)][1:]
    others = [along_y[a] + along_x[b] + cores[c] for a, b, c in steps]
    above = [lax.rem(deep + i, nd) for i in range(1, nd)]

    barrier = pltpu.get_barrier_semaphore()
    for peer in others:
        pl.semaphore_signal(
            barrier, inc=1, device_id={"north": peer, "deep": deep}, device_id_type=MESH
        )
    for peer in above:
        pl.semaphore_signal(
            barrier, inc=1, device_id={"north": me, "deep": peer}, device_id_type=MESH
        )

    def transform_x(y, first, last, high, low):
        span = nn * rows
        pick = pl.ds(first * span, (last - first) * span)
        result = product(hx[0, pick, :], hx[1, pick, :], high, low, transposed=True)
        for c in range(first, last):
            part = result[(c - first) * span : (c - first + 1) * span]
            for t in range(tiles):
                sbuf[c, t, pl.ds(y, span, stride=ny), :] = part[:, t * 128 : (t + 1) * 128]

    def north(c, slot, tile, start):
        pick = pl.ds(0, tiles) if tile is None else pl.ds(tile, 1)

        def copy(source, target, peer):
            return pltpu.make_async_remote_copy(
                src_ref=source,
                dst_ref=target,
                send_sem=ssem.at[slot],
                recv_sem=rsem.at[slot],
                device_id={"north": peer, "deep": deep},
                device_id_type=MESH,
            )

        if not start:
            everything = rbuf.at[c, pick, pl.ds(0, nn - 1)]
            return copy(everything, everything, me)
        for peer in others:
            copy(sbuf.at[c, pick, pl.ds(pl.multiple_of(peer * piece, piece), piece)], rbuf.at[c, pick, me], peer).start()
        rbuf[c, pick, me] = sbuf[c, pick, pl.ds(pl.multiple_of(me * piece, piece), piece), :]

    def vertical(c, slot, tile, start):
        pick = pl.ds(0, tiles) if tile is None else pl.ds(tile, 1)

        def copy(source, target, peer):
            return pltpu.make_async_remote_copy(
                src_ref=source,
                dst_ref=target,
                send_sem=dssem.at[slot],
                recv_sem=drsem.at[slot],
                device_id={"north": me, "deep": peer},
                device_id_type=MESH,
            )

        if not start:
            everything = drecv.at[c, pl.ds(0, nd - 1), pick]
            return copy(everything, everything, deep)
        for peer in above:
            copy(dsend.at[c, peer, pick], drecv.at[c, deep, pick], peer).start()
        drecv[c, deep, pick] = dsend[c, deep, pick]

    def group_x(first, last):
        @pl.loop(0, ny)
        def _(y):
            transform_x(y, first, last, vhi[y], vlo[y])

        @pl.loop(first, last)
        def _(c):
            north(c, c, None, True)

    def stage_y(c, slot, tile=None):
        north(c, slot, tile, False).wait_recv()
        span = range(tiles) if tile is None else (tile,)
        for j in range(rows):
            columns = [rbuf[c, t, :, pl.ds(j * ny, ny), :].reshape(full_y, 128) for t in span]
            high, low = split(jnp.concatenate(columns, axis=1))
            result = product(hy[0], hy[1], high, low)
            for d in range(nd):
                for k, t in enumerate(span):
                    dsend[c, d, t, j] = result[d * share_y : (d + 1) * share_y, k * 128 : (k + 1) * 128]
        vertical(c, slot, tile, True)

    lower = lax.broadcasted_iota(jnp.int32, (share_y, 128), 1) < nz

    def stage_z(c):
        for j in range(rows):
            lines = []
            for t in range(tiles):
                parts = [drecv[c, d, t, j] for d in range(nd)]
                turned = [pltpu.roll(p, nz, 1) for p in parts]
                even = [jnp.where(lower, parts[d], turned[d + 1]) for d in range(0, nd, 2)]
                odd = [jnp.where(lower, turned[d], parts[d + 1]) for d in range(0, nd, 2)]
                lines.append(jnp.concatenate(even, axis=1))
                lines.append(jnp.concatenate(odd, axis=1))
            high, low = split(jnp.concatenate(lines, axis=0))
            result = product(high, low, hy[0], hy[1])
            old = [result[f * share_y : (f + 1) * share_y] for f in range(fields)]
            x = c * rows + j
            weight = 1.0 / (1.0 + (sym_x[me * share_x + x] + syz[...]))
            rest = 1.0 - weight
            for a in range(fields):
                mixed = coupling[a, 0] * old[0]
                for b in range(1, fields):
                    mixed = mixed + coupling[a, b] * old[b]
                out[a, x] = weight * old[a] + rest * mixed

    loads[0].wait()
    for y in range(0, ny, 2):
        load_v[y].wait()
        load_v[y + 1].wait()
        for k in (y, y + 1):
            high, low = split(vbuf[k].reshape(wide, nx))
            vhi[k] = high
            vlo[k] = low
            transform_x(k, 0, FIRST, high, low)
    for copy in loads[1:]:
        copy.start()
    pl.semaphore_wait(barrier, nn - 1 + nd - 1)
    north(0, 0, 0, True)
    north(0, chunks, 1, True)
    for c in range(1, FIRST):
        north(c, c, None, True)

    done = 1
    for item in PLAN:
        if item == "start":
            for copy in loads[1:]:
                copy.wait()
            stage_y(0, 0, 0)
            stage_y(0, chunks, 1)
        elif isinstance(item, tuple):
            group_x(*item)
        else:
            stage_y(item, item)
            done = item + 1

    lane = lax.broadcasted_iota(jnp.int32, (share_y, full_y), 1)
    row = lax.broadcasted_iota(jnp.int32, (share_y, full_y), 0)
    mine = jnp.where(lane == row + deep * share_y, sym_y[...], 0.0)
    syz[...] = jnp.sum(mine, axis=1, keepdims=True) + sym_z[...]

    @pl.loop(done, LAG)
    def _(c):
        stage_y(c, c)

    vertical(0, 0, 0, False).wait_recv()
    vertical(0, chunks, 1, False).wait_recv()
    stage_y(LAG, LAG)
    stage_z(0)

    @pl.loop(LAG + 1, chunks)
    def _(c):
        stage_y(c, c)
        vertical(c - LAG, c - LAG, None, False).wait_recv()
        stage_z(c - LAG)

    @pl.loop(chunks - LAG, chunks)
    def _(c):
        vertical(c, c, None, False).wait_recv()
        stage_z(c)

    north(0, 0, 0, False).wait_send()
    north(0, chunks, 1, False).wait_send()
    vertical(0, 0, 0, False).wait_send()
    vertical(0, chunks, 1, False).wait_send()

    @pl.loop(1, chunks)
    def _(c):
        north(c, c, None, False).wait_send()
        vertical(c, c, None, False).wait_send()


def on_device(nn, nd, velocity, coupling, symbol_x, symbol_y, symbol_z):
    fields, nx, ny, nz = velocity.shape
    share_x = nx // nn
    rows = share_x // CHUNKS
    full_y, full_z = ny * nn, nz * nd
    share_y = full_y // nd
    wide = fields * nz
    tiles = wide // 128
    order = np.arange(nx).reshape(nn, CHUNKS, rows).transpose(1, 0, 2).reshape(-1)
    table_x = jnp.asarray(two_parts(basis_table(nx)[order]))
    table_y = jnp.asarray(two_parts(basis_table(full_y)))
    dma = pltpu.SemaphoreType.DMA
    return pl.pallas_call(
        functools.partial(kernel, nn, nd),
        out_shape=jax.ShapeDtypeStruct((fields, share_x, share_y, full_z), F32),
        in_specs=[pl.BlockSpec(memory_space=pltpu.MemorySpace.HBM)] * 7,
        out_specs=pl.BlockSpec(memory_space=pltpu.VMEM),
        scratch_shapes=[
            pltpu.VMEM((ny, fields, nz, nx), F32),
            pltpu.VMEM((ny, wide, nx), BF16),
            pltpu.VMEM((ny, wide, nx), BF16),
            pltpu.VMEM((2, nx, nx), BF16),
            pltpu.VMEM((2, full_y, full_y), BF16),
            pltpu.VMEM((CHUNKS, tiles, nn * rows * ny, 128), F32),
            pltpu.VMEM((CHUNKS, tiles, nn, rows * ny, 128), F32),
            pltpu.VMEM((CHUNKS, nd, tiles, rows, share_y, 128), F32),
            pltpu.VMEM((CHUNKS, nd, tiles, rows, share_y, 128), F32),
            pltpu.VMEM((share_y, full_z), F32),
            pltpu.SMEM((fields, fields), F32),
            pltpu.SMEM((nx,), F32),
            pltpu.VMEM((1, full_y), F32),
            pltpu.VMEM((1, full_z), F32),
            dma((ny,)), dma((6,)),
            dma((CHUNKS + 1,)), dma((CHUNKS + 1,)), dma((CHUNKS + 1,)), dma((CHUNKS + 1,)),
        ],
        compiler_params=pltpu.CompilerParams(
            collective_id=0, has_side_effects=True, vmem_limit_bytes=32 << 20
        ),
    )(*(
        pltpu.with_memory_space_constraint(array, pltpu.MemorySpace.HBM)
        for array in (
            jnp.transpose(velocity, (0, 2, 3, 1)), table_x, table_y, coupling, symbol_x,
            symbol_y.reshape(1, full_y), symbol_z.reshape(1, full_z),
        )
    ))


def solution(mesh):
    placed = (P(None, None, "north", "deep"), P(), P(), P(), P())
    return jax.shard_map(
        functools.partial(on_device, mesh.shape["north"], mesh.shape["deep"]),
        mesh=mesh,
        in_specs=placed,
        out_specs=P(None, "north", "deep", None),
        check_vma=False,
    )
```

```python
import functools

import jax
import jax.numpy as jnp
import numpy as np
from jax import lax
from jax.experimental import pallas as pl
from jax.experimental.pallas import tpu as pltpu
from jax.sharding import PartitionSpec as P

MESH = pl.DeviceIdType.MESH
F32, BF16 = jnp.float32, jnp.bfloat16
CHUNKS = 16
FIRST = 3
LAG = 3
AHEAD = 6
EARLY = 6


def basis_table(count):
    rank = np.arange(1, count + 1)
    turns = (rank[:, None] * rank[None, :]) % (2 * count + 2)
    return np.sin(np.pi * turns / (count + 1)) * np.sqrt(2.0 / (count + 1))


def two_parts(table):
    high = table.astype(BF16)
    low = (table - high.astype(np.float64)).astype(BF16)
    return np.stack([high, low])


def split(values):
    high = values.astype(BF16)
    return high, (values - high.astype(F32)).astype(BF16)


def dot(a, b, transposed=False):
    dims = (((1,), (1 if transposed else 0,)), ((), ()))
    return lax.dot_general(a, b, dims, preferred_element_type=F32)


def product(a_high, a_low, b_high, b_low, transposed=False):
    count = a_high.shape[0]
    both = dot(jnp.concatenate([a_high, a_low], axis=0), b_high, transposed)
    return both[:count] + (both[count:] + dot(a_high, b_low, transposed))


def kernel(
    nn, nd, v_hbm, hx_hbm, hy_hbm, coupling_hbm, sym_x_hbm, sym_y_hbm, sym_z_hbm, out,
    vbuf, vhi, vlo, hx, hy, sbuf, rbuf, dsend, drecv, syz, coupling, sym_x, sym_y, sym_z,
    vsem, hsem, ssem, rsem, dssem, drsem,
):
    fields, ny, nz, nx = v_hbm.shape
    chunks = sbuf.shape[0]
    share_x = nx // nn
    rows = share_x // chunks
    wide = fields * nz
    tiles = wide // 128
    full_y = nn * ny
    share_y = full_y // nd
    piece = rows * ny
    me, deep = lax.axis_index("north"), lax.axis_index("deep")

    loads = [
        pltpu.make_async_copy(a, b, hsem.at[k])
        for k, (a, b) in enumerate((
            (hx_hbm, hx), (hy_hbm, hy), (coupling_hbm, coupling), (sym_x_hbm, sym_x),
            (sym_y_hbm, sym_y), (sym_z_hbm, sym_z),
        ))
    ]
    load_v = [pltpu.make_async_copy(v_hbm.at[:, y], vbuf.at[y], vsem.at[y]) for y in range(ny)]
    loads[0].start()
    for copy in load_v:
        copy.start()

    along_y = [lax.rem(me // 8 + i, 4) * 8 for i in range(4)]
    along_x = [lax.rem(me // 2 + i, 4) * 2 for i in range(4)]
    cores = [lax.rem(me + i, 2) for i in range(2)]
    steps = [(a, b, c) for a in range(4) for b in range(4) for c in range(2)][1:]
    others = [along_y[a] + along_x[b] + cores[c] for a, b, c in steps]
    above = [lax.rem(deep + i, nd) for i in range(1, nd)]

    barrier = pltpu.get_barrier_semaphore()
    for peer in others:
        pl.semaphore_signal(
            barrier, inc=1, device_id={"north": peer, "deep": deep}, device_id_type=MESH
        )
    for peer in above:
        pl.semaphore_signal(
            barrier, inc=1, device_id={"north": me, "deep": peer}, device_id_type=MESH
        )

    def transform_x(y, first, last, high, low):
        span = nn * rows
        pick = pl.ds(first * span, (last - first) * span)
        result = product(hx[0, pick, :], hx[1, pick, :], high, low, transposed=True)
        for c in range(first, last):
            part = result[(c - first) * span : (c - first + 1) * span]
            for t in range(tiles):
                sbuf[c, t, pl.ds(y, span, stride=ny), :] = part[:, t * 128 : (t + 1) * 128]

    def north(c, slot, tile, start):
        pick = pl.ds(0, tiles) if tile is None else pl.ds(tile, 1)

        def copy(source, target, peer):
            return pltpu.make_async_remote_copy(
                src_ref=source,
                dst_ref=target,
                send_sem=ssem.at[slot],
                recv_sem=rsem.at[slot],
                device_id={"north": peer, "deep": deep},
                device_id_type=MESH,
            )

        if not start:
            everything = rbuf.at[c, pick, pl.ds(0, nn - 1)]
            return copy(everything, everything, me)
        for peer in others:
            copy(sbuf.at[c, pick, pl.ds(pl.multiple_of(peer * piece, piece), piece)], rbuf.at[c, pick, me], peer).start()
        rbuf[c, pick, me] = sbuf[c, pick, pl.ds(pl.multiple_of(me * piece, piece), piece), :]

    def vertical(c, slot, tile, start):
        pick = pl.ds(0, tiles) if tile is None else pl.ds(tile, 1)

        def copy(source, target, peer):
            return pltpu.make_async_remote_copy(
                src_ref=source,
                dst_ref=target,
                send_sem=dssem.at[slot],
                recv_sem=drsem.at[slot],
                device_id={"north": me, "deep": peer},
                device_id_type=MESH,
            )

        if not start:
            everything = drecv.at[c, pl.ds(0, nd - 1), pick]
            return copy(everything, everything, deep)
        for peer in above:
            copy(dsend.at[c, peer, pick], drecv.at[c, deep, pick], peer).start()
        drecv[c, deep, pick] = dsend[c, deep, pick]

    def rest_x(start, stop):
        @pl.loop(start, stop)
        def _(y):
            transform_x(y, FIRST, chunks, vhi[y], vlo[y])

    def send(c):
        if not isinstance(c, int):
            north(c, c, None, True)
        elif c in (0, chunks - 1):
            north(c, c, 0, True)
            north(c, chunks + (c > 0), 1, True)
        elif c < chunks:
            north(c, c, None, True)

    def stage_y(c, slot, tile=None):
        north(c, slot, tile, False).wait_recv()
        span = range(tiles) if tile is None else (tile,)
        for j in range(rows):
            columns = [rbuf[c, t, :, pl.ds(j * ny, ny), :].reshape(full_y, 128) for t in span]
            high, low = split(jnp.concatenate(columns, axis=1))
            result = product(hy[0], hy[1], high, low)
            for d in range(nd):
                for k, t in enumerate(span):
                    dsend[c, d, t, j] = result[d * share_y : (d + 1) * share_y, k * 128 : (k + 1) * 128]
        vertical(c, slot, tile, True)

    lower = lax.broadcasted_iota(jnp.int32, (share_y, 128), 1) < nz

    def stage_z(c):
        for j in range(rows):
            lines = []
            for t in range(tiles):
                parts = [drecv[c, d, t, j] for d in range(nd)]
                turned = [pltpu.roll(p, nz, 1) for p in parts]
                even = [jnp.where(lower, parts[d], turned[d + 1]) for d in range(0, nd, 2)]
                odd = [jnp.where(lower, turned[d], parts[d + 1]) for d in range(0, nd, 2)]
                lines.append(jnp.concatenate(even, axis=1))
                lines.append(jnp.concatenate(odd, axis=1))
            high, low = split(jnp.concatenate(lines, axis=0))
            result = product(high, low, hy[0], hy[1])
            old = [result[f * share_y : (f + 1) * share_y] for f in range(fields)]
            x = c * rows + j
            weight = 1.0 / (1.0 + (sym_x[me * share_x + x] + syz[...]))
            rest = 1.0 - weight
            for a in range(fields):
                mixed = coupling[a, 0] * old[0]
                for b in range(1, fields):
                    mixed = mixed + coupling[a, b] * old[b]
                out[a, x] = weight * old[a] + rest * mixed

    loads[0].wait()
    for y in range(0, ny, 2):
        load_v[y].wait()
        load_v[y + 1].wait()
        for k in (y, y + 1):
            high, low = split(vbuf[k].reshape(wide, nx))
            vhi[k] = high
            vlo[k] = low
            transform_x(k, 0, FIRST, high, low)
    for copy in loads[1:]:
        copy.start()
    pl.semaphore_wait(barrier, nn - 1 + nd - 1)
    for c in range(FIRST):
        send(c)
    rest_x(0, EARLY)
    for copy in loads[1:]:
        copy.wait()
    stage_y(0, 0, 0)
    rest_x(EARLY, EARLY + 1)
    stage_y(0, chunks, 1)
    rest_x(EARLY + 1, ny)

    @pl.loop(FIRST, AHEAD)
    def _(c):
        send(c)

    lane = lax.broadcasted_iota(jnp.int32, (share_y, full_y), 1)
    row = lax.broadcasted_iota(jnp.int32, (share_y, full_y), 0)
    mine = jnp.where(lane == row + deep * share_y, sym_y[...], 0.0)
    syz[...] = jnp.sum(mine, axis=1, keepdims=True) + sym_z[...]

    @pl.loop(1, LAG)
    def _(c):
        stage_y(c, c)
        send(c + AHEAD - 1)

    vertical(0, 0, 0, False).wait_recv()
    vertical(0, chunks, 1, False).wait_recv()
    stage_y(LAG, LAG)
    send(LAG + AHEAD - 1)
    stage_z(0)

    @pl.loop(LAG + 1, chunks - AHEAD)
    def _(c):
        stage_y(c, c)
        send(c + AHEAD - 1)
        vertical(c - LAG, c - LAG, None, False).wait_recv()
        stage_z(c - LAG)

    send(chunks - 1)

    @pl.loop(chunks - AHEAD, chunks - 1)
    def _(c):
        stage_y(c, c)
        vertical(c - LAG, c - LAG, None, False).wait_recv()
        stage_z(c - LAG)

    stage_y(chunks - 1, chunks - 1, 0)
    stage_y(chunks - 1, chunks + 1, 1)

    @pl.loop(chunks - 1 - LAG, chunks - 1)
    def _(c):
        vertical(c, c, None, False).wait_recv()
        stage_z(c)

    vertical(chunks - 1, chunks - 1, 0, False).wait_recv()
    vertical(chunks - 1, chunks + 1, 1, False).wait_recv()
    stage_z(chunks - 1)

    for c, slot, tile in ((0, 0, 0), (0, chunks, 1), (chunks - 1, chunks - 1, 0), (chunks - 1, chunks + 1, 1)):
        north(c, slot, tile, False).wait_send()
        vertical(c, slot, tile, False).wait_send()

    @pl.loop(1, chunks - 1)
    def _(c):
        north(c, c, None, False).wait_send()
        vertical(c, c, None, False).wait_send()


def on_device(nn, nd, velocity, coupling, symbol_x, symbol_y, symbol_z):
    fields, nx, ny, nz = velocity.shape
    share_x = nx // nn
    rows = share_x // CHUNKS
    full_y, full_z = ny * nn, nz * nd
    share_y = full_y // nd
    wide = fields * nz
    tiles = wide // 128
    order = np.arange(nx).reshape(nn, CHUNKS, rows).transpose(1, 0, 2).reshape(-1)
    table_x = jnp.asarray(two_parts(basis_table(nx)[order]))
    table_y = jnp.asarray(two_parts(basis_table(full_y)))
    dma = pltpu.SemaphoreType.DMA
    return pl.pallas_call(
        functools.partial(kernel, nn, nd),
        out_shape=jax.ShapeDtypeStruct((fields, share_x, share_y, full_z), F32),
        in_specs=[pl.BlockSpec(memory_space=pltpu.MemorySpace.HBM)] * 7,
        out_specs=pl.BlockSpec(memory_space=pltpu.VMEM),
        scratch_shapes=[
            pltpu.VMEM((ny, fields, nz, nx), F32),
            pltpu.VMEM((ny, wide, nx), BF16),
            pltpu.VMEM((ny, wide, nx), BF16),
            pltpu.VMEM((2, nx, nx), BF16),
            pltpu.VMEM((2, full_y, full_y), BF16),
            pltpu.VMEM((CHUNKS, tiles, nn * rows * ny, 128), F32),
            pltpu.VMEM((CHUNKS, tiles, nn, rows * ny, 128), F32),
            pltpu.VMEM((CHUNKS, nd, tiles, rows, share_y, 128), F32),
            pltpu.VMEM((CHUNKS, nd, tiles, rows, share_y, 128), F32),
            pltpu.VMEM((share_y, full_z), F32),
            pltpu.SMEM((fields, fields), F32),
            pltpu.SMEM((nx,), F32),
            pltpu.VMEM((1, full_y), F32),
            pltpu.VMEM((1, full_z), F32),
            dma((ny,)), dma((6,)),
            dma((CHUNKS + 2,)), dma((CHUNKS + 2,)), dma((CHUNKS + 2,)), dma((CHUNKS + 2,)),
        ],
        compiler_params=pltpu.CompilerParams(
            collective_id=0, has_side_effects=True, vmem_limit_bytes=32 << 20
        ),
    )(*(
        pltpu.with_memory_space_constraint(array, pltpu.MemorySpace.HBM)
        for array in (
            jnp.transpose(velocity, (0, 2, 3, 1)), table_x, table_y, coupling, symbol_x,
            symbol_y.reshape(1, full_y), symbol_z.reshape(1, full_z),
        )
    ))


def solution(mesh):
    placed = (P(None, None, "north", "deep"), P(), P(), P(), P())
    return jax.shard_map(
        functools.partial(on_device, mesh.shape["north"], mesh.shape["deep"]),
        mesh=mesh,
        in_specs=placed,
        out_specs=P(None, "north", "deep", None),
        check_vma=False,
    )
```

```python
import functools

import jax
import jax.numpy as jnp
import numpy as np
from jax import lax
from jax.experimental import pallas as pl
from jax.experimental.pallas import tpu as pltpu
from jax.sharding import PartitionSpec as P

MESH = pl.DeviceIdType.MESH
F32, BF16 = jnp.float32, jnp.bfloat16
CHUNKS = 16
FIRST = 3
LAG = 3
AHEAD = 4


def basis_table(count):
    rank = np.arange(1, count + 1)
    turns = (rank[:, None] * rank[None, :]) % (2 * count + 2)
    return np.sin(np.pi * turns / (count + 1)) * np.sqrt(2.0 / (count + 1))


def two_parts(table):
    high = table.astype(BF16)
    low = (table - high.astype(np.float64)).astype(BF16)
    return np.stack([high, low])


def split(values):
    high = values.astype(BF16)
    return high, (values - high.astype(F32)).astype(BF16)


def dot(a, b, transposed=False):
    dims = (((1,), (1 if transposed else 0,)), ((), ()))
    return lax.dot_general(a, b, dims, preferred_element_type=F32)


def product(a_high, a_low, b_high, b_low, transposed=False):
    count = a_high.shape[0]
    both = dot(jnp.concatenate([a_high, a_low], axis=0), b_high, transposed)
    return both[:count] + (both[count:] + dot(a_high, b_low, transposed))


def kernel(
    nn, nd, v_hbm, hx_hbm, hy_hbm, coupling_hbm, sym_x_hbm, sym_y_hbm, sym_z_hbm, out,
    vbuf, vhi, vlo, hx, hy, sbuf, rbuf, dsend, drecv, syz, coupling, sym_x, sym_y, sym_z,
    vsem, hsem, ssem, rsem, dssem, drsem,
):
    fields, ny, nz, nx = v_hbm.shape
    chunks = sbuf.shape[0]
    share_x = nx // nn
    rows = share_x // chunks
    wide = fields * nz
    tiles = wide // 128
    full_y = nn * ny
    share_y = full_y // nd
    piece = rows * ny
    me, deep = lax.axis_index("north"), lax.axis_index("deep")

    loads = [
        pltpu.make_async_copy(a, b, hsem.at[k])
        for k, (a, b) in enumerate((
            (hx_hbm, hx), (hy_hbm, hy), (coupling_hbm, coupling), (sym_x_hbm, sym_x),
            (sym_y_hbm, sym_y), (sym_z_hbm, sym_z),
        ))
    ]
    load_v = [pltpu.make_async_copy(v_hbm.at[:, y], vbuf.at[y], vsem.at[y]) for y in range(ny)]
    loads[0].start()
    for copy in load_v:
        copy.start()

    along_y = [lax.rem(me // 8 + i, 4) * 8 for i in range(4)]
    along_x = [lax.rem(me // 2 + i, 4) * 2 for i in range(4)]
    cores = [lax.rem(me + i, 2) for i in range(2)]
    steps = [(a, b, c) for a in range(4) for b in range(4) for c in range(2)][1:]
    others = [along_y[a] + along_x[b] + cores[c] for a, b, c in steps]
    hops = [min(a, 4 - a) + min(b, 4 - b) for a, b, c in steps]
    farthest = [others[k] for k in sorted(range(len(steps)), key=lambda k: -hops[k])]
    above = [lax.rem(deep + i, nd) for i in (1, 2, 3)]

    barrier = pltpu.get_barrier_semaphore()
    for peer in farthest:
        pl.semaphore_signal(
            barrier, inc=1, device_id={"north": peer, "deep": deep}, device_id_type=MESH
        )
    for peer in above:
        pl.semaphore_signal(
            barrier, inc=1, device_id={"north": me, "deep": peer}, device_id_type=MESH
        )

    def transform_x(y, first, last, high, low):
        span = nn * rows
        pick = pl.ds(first * span, (last - first) * span)
        result = product(hx[0, pick, :], hx[1, pick, :], high, low, transposed=True)
        for c in range(first, last):
            part = result[(c - first) * span : (c - first + 1) * span]
            for t in range(tiles):
                sbuf[c, t, pl.ds(y, span, stride=ny), :] = part[:, t * 128 : (t + 1) * 128]

    def north(c, t, start):
        slot = c * tiles + t

        def copy(source, target, peer):
            return pltpu.make_async_remote_copy(
                src_ref=source,
                dst_ref=target,
                send_sem=ssem.at[slot],
                recv_sem=rsem.at[slot],
                device_id={"north": peer, "deep": deep},
                device_id_type=MESH,
            )

        if not start:
            everything = rbuf.at[c, t, pl.ds(0, nn - 1)]
            return copy(everything, everything, me)
        for peer in farthest:
            copy(sbuf.at[c, t, pl.ds(pl.multiple_of(peer * piece, piece), piece)], rbuf.at[c, t, me], peer).start()
        rbuf[c, t, me] = sbuf[c, t, pl.ds(pl.multiple_of(me * piece, piece), piece), :]

    def vertical(c, t, start):
        slot = c * tiles + t

        def copy(source, target, peer):
            return pltpu.make_async_remote_copy(
                src_ref=source,
                dst_ref=target,
                send_sem=dssem.at[slot],
                recv_sem=drsem.at[slot],
                device_id={"north": me, "deep": peer},
                device_id_type=MESH,
            )

        if not start:
            everything = drecv.at[c, t, pl.ds(0, nd - 1)]
            return copy(everything, everything, deep)
        for peer in above:
            copy(dsend.at[c, t, peer], drecv.at[c, t, deep], peer).start()
        drecv[c, t, deep] = dsend[c, t, deep]

    def rest_x(start, stop):
        @pl.loop(start, stop)
        def _(y):
            transform_x(y, FIRST, chunks, vhi[y], vlo[y])

    def stage_y(c, t):
        north(c, t, False).wait_recv()
        for j in range(rows):
            high, low = split(rbuf[c, t, :, pl.ds(j * ny, ny), :].reshape(full_y, 128))
            result = product(hy[0], hy[1], high, low)
            for d in range(nd):
                dsend[c, t, d, j] = result[d * share_y : (d + 1) * share_y]
        vertical(c, t, True)

    lower = lax.broadcasted_iota(jnp.int32, (share_y, 128), 1) < nz

    def stage_z(c):
        for t in range(tiles):
            vertical(c, t, False).wait_recv()
        for j in range(rows):
            lines = []
            for t in range(tiles):
                parts = [drecv[c, t, d, j] for d in range(nd)]
                turned = [pltpu.roll(p, nz, 1) for p in parts]
                even = [jnp.where(lower, parts[d], turned[d + 1]) for d in range(0, nd, 2)]
                odd = [jnp.where(lower, turned[d], parts[d + 1]) for d in range(0, nd, 2)]
                lines.append(jnp.concatenate(even, axis=1))
                lines.append(jnp.concatenate(odd, axis=1))
            high, low = split(jnp.concatenate(lines, axis=0))
            result = product(high, low, hy[0], hy[1])
            old = [result[f * share_y : (f + 1) * share_y] for f in range(fields)]
            x = c * rows + j
            weight = 1.0 / (1.0 + (sym_x[me * share_x + x] + syz[...]))
            rest = 1.0 - weight
            for a in range(fields):
                mixed = coupling[a, 0] * old[0]
                for b in range(1, fields):
                    mixed = mixed + coupling[a, b] * old[b]
                out[a, x] = weight * old[a] + rest * mixed

    loads[0].wait()
    for y in range(0, ny, 2):
        load_v[y].wait()
        load_v[y + 1].wait()
        for k in (y, y + 1):
            high, low = split(vbuf[k].reshape(wide, nx))
            vhi[k] = high
            vlo[k] = low
            transform_x(k, 0, FIRST, high, low)
    for copy in loads[1:]:
        copy.start()
    pl.semaphore_wait(barrier, nn - 1 + nd - 1)
    north(0, 0, True)
    rest_x(0, 2)
    north(0, 1, True)
    rest_x(2, 4)
    north(1, 0, True)
    north(1, 1, True)
    rest_x(4, 7)
    for copy in loads[1:]:
        copy.wait()
    stage_y(0, 0)
    north(2, 0, True)
    north(2, 1, True)
    stage_y(0, 1)
    rest_x(7, 8)
    for c in range(FIRST, AHEAD):
        for t in range(tiles):
            north(c, t, True)

    lane = lax.broadcasted_iota(jnp.int32, (share_y, full_y), 1)
    row = lax.broadcasted_iota(jnp.int32, (share_y, full_y), 0)
    mine = jnp.where(lane == row + deep * share_y, sym_y[...], 0.0)
    syz[...] = jnp.sum(mine, axis=1, keepdims=True) + sym_z[...]

    def step(c, more, ready):
        stage_y(c, 0)
        if more:
            north(c + AHEAD - 1, 0, True)
        if ready:
            stage_z(c - LAG)
        stage_y(c, 1)
        if more:
            north(c + AHEAD - 1, 1, True)

    for first, last, more, ready in (
        (1, LAG, True, False),
        (LAG, chunks - AHEAD + 1, True, True),
        (chunks - AHEAD + 1, chunks, False, True),
    ):
        @pl.loop(first, last)
        def _(c):
            step(c, more, ready)

    @pl.loop(chunks - LAG, chunks)
    def _(c):
        stage_z(c)

    @pl.loop(0, chunks)
    def _(c):
        for t in range(tiles):
            north(c, t, False).wait_send()
            vertical(c, t, False).wait_send()


def on_device(nn, nd, velocity, coupling, symbol_x, symbol_y, symbol_z):
    fields, nx, ny, nz = velocity.shape
    share_x = nx // nn
    rows = share_x // CHUNKS
    full_y, full_z = ny * nn, nz * nd
    share_y = full_y // nd
    wide = fields * nz
    tiles = wide // 128
    order = np.arange(nx).reshape(nn, CHUNKS, rows).transpose(1, 0, 2).reshape(-1)
    table_x = jnp.asarray(two_parts(basis_table(nx)[order]))
    table_y = jnp.asarray(two_parts(basis_table(full_y)))
    dma = pltpu.SemaphoreType.DMA
    return pl.pallas_call(
        functools.partial(kernel, nn, nd),
        out_shape=jax.ShapeDtypeStruct((fields, share_x, share_y, full_z), F32),
        in_specs=[pl.BlockSpec(memory_space=pltpu.MemorySpace.HBM)] * 7,
        out_specs=pl.BlockSpec(memory_space=pltpu.VMEM),
        scratch_shapes=[
            pltpu.VMEM((ny, fields, nz, nx), F32),
            pltpu.VMEM((ny, wide, nx), BF16),
            pltpu.VMEM((ny, wide, nx), BF16),
            pltpu.VMEM((2, nx, nx), BF16),
            pltpu.VMEM((2, full_y, full_y), BF16),
            pltpu.VMEM((CHUNKS, tiles, nn * rows * ny, 128), F32),
            pltpu.VMEM((CHUNKS, tiles, nn, rows * ny, 128), F32),
            pltpu.VMEM((CHUNKS, tiles, nd, rows, share_y, 128), F32),
            pltpu.VMEM((CHUNKS, tiles, nd, rows, share_y, 128), F32),
            pltpu.VMEM((share_y, full_z), F32),
            pltpu.SMEM((fields, fields), F32),
            pltpu.SMEM((nx,), F32),
            pltpu.VMEM((1, full_y), F32),
            pltpu.VMEM((1, full_z), F32),
            dma((ny,)), dma((6,)),
            dma((CHUNKS * tiles,)), dma((CHUNKS * tiles,)), dma((CHUNKS * tiles,)), dma((CHUNKS * tiles,)),
        ],
        compiler_params=pltpu.CompilerParams(
            collective_id=0, has_side_effects=True, vmem_limit_bytes=32 << 20
        ),
    )(*(
        pltpu.with_memory_space_constraint(array, pltpu.MemorySpace.HBM)
        for array in (
            jnp.transpose(velocity, (0, 2, 3, 1)), table_x, table_y, coupling, symbol_x,
            symbol_y.reshape(1, full_y), symbol_z.reshape(1, full_z),
        )
    ))


def solution(mesh):
    placed = (P(None, None, "north", "deep"), P(), P(), P(), P())
    return jax.shard_map(
        functools.partial(on_device, mesh.shape["north"], mesh.shape["deep"]),
        mesh=mesh,
        in_specs=placed,
        out_specs=P(None, "north", "deep", None),
        check_vma=False,
    )
```

```python
import functools

import jax
import jax.numpy as jnp
import numpy as np
from jax import lax
from jax.experimental import pallas as pl
from jax.experimental.pallas import tpu as pltpu
from jax.sharding import PartitionSpec as P

MESH = pl.DeviceIdType.MESH
F32, BF16 = jnp.float32, jnp.bfloat16
CHUNKS = 16
FIRST = 3
LAG = 3
AHEAD = 4


def basis_table(count):
    rank = np.arange(1, count + 1)
    turns = (rank[:, None] * rank[None, :]) % (2 * count + 2)
    return np.sin(np.pi * turns / (count + 1)) * np.sqrt(2.0 / (count + 1))


def two_parts(table):
    high = table.astype(BF16)
    low = (table - high.astype(np.float64)).astype(BF16)
    return np.stack([high, low])


def split(values):
    high = values.astype(BF16)
    return high, (values - high.astype(F32)).astype(BF16)


def dot(a, b, transposed=False):
    dims = (((1,), (1 if transposed else 0,)), ((), ()))
    return lax.dot_general(a, b, dims, preferred_element_type=F32)


def product(a_high, a_low, b_high, b_low, transposed=False):
    count = a_high.shape[0]
    both = dot(jnp.concatenate([a_high, a_low], axis=0), b_high, transposed)
    return both[:count] + (both[count:] + dot(a_high, b_low, transposed))


def transform_z(pieces, table, nz):
    lower = lax.broadcasted_iota(jnp.int32, pieces[0][0].shape, 1) < nz
    lines = []
    for parts in pieces:
        turned = [pltpu.roll(p, nz, 1) for p in parts]
        pairs = range(0, len(parts), 2)
        even = [jnp.where(lower, parts[d], turned[d + 1]) for d in pairs]
        odd = [jnp.where(lower, turned[d], parts[d + 1]) for d in pairs]
        lines.append(jnp.concatenate(even, axis=1))
        lines.append(jnp.concatenate(odd, axis=1))
    high, low = split(jnp.concatenate(lines, axis=0))
    result = product(high, low, table[0], table[1])
    share = pieces[0][0].shape[0]
    return [result[f * share : (f + 1) * share] for f in range(len(lines))]


def mixed_with(old, coupling, weight):
    rest = 1.0 - weight
    for a in range(len(old)):
        mixed = coupling(a, 0) * old[0]
        for b in range(1, len(old)):
            mixed = mixed + coupling(a, b) * old[b]
        yield weight * old[a] + rest * mixed


def finish(nz, most, last, table, weight, coupling, result, final, sem):
    fields, share_x = most.shape[:2]
    copies = [
        pltpu.make_async_copy(most.at[f, pl.ds(0, share_x - 1)], result.at[f, pl.ds(0, share_x - 1)], sem.at[f])
        for f in range(fields)
    ]
    for copy in copies:
        copy.start()
    tiles, nd = last.shape[:2]
    old = transform_z([[last[t, d] for d in range(nd)] for t in range(tiles)], table, nz)

    def factor(a, b):
        return coupling[pl.ds(a * fields + b, 1), :]

    for a, values in enumerate(mixed_with(old, factor, weight[...])):
        final[a] = values
        copies.append(pltpu.make_async_copy(final.at[a], result.at[a, share_x - 1], sem.at[fields + a]))
        copies[-1].start()
    for copy in copies:
        copy.wait()


def kernel(
    nn, nd, v_hbm, hx_hbm, hy_hbm, coupling_hbm, sym_x_hbm, sym_y_hbm, sym_z_hbm, out, tail, table, weight, mixing,
    vbuf, vhi, vlo, hx, hy, sbuf, rbuf, dsend, drecv, syz, coupling, sym_x, sym_y, sym_z,
    vsem, hsem, ssem, rsem, dssem, drsem,
):
    fields, ny, nz, nx = v_hbm.shape
    chunks = sbuf.shape[0]
    share_x = nx // nn
    rows = share_x // chunks
    wide = fields * nz
    tiles = wide // 128
    full_y = nn * ny
    share_y = full_y // nd
    piece = rows * ny
    me, deep = lax.axis_index("north"), lax.axis_index("deep")

    soon = FIRST * nn * rows
    loads = [
        pltpu.make_async_copy(a, b, hsem.at[k])
        for k, (a, b) in enumerate((
            (hx_hbm.at[:, pl.ds(0, soon)], hx.at[:, pl.ds(0, soon)]),
            (hx_hbm.at[:, pl.ds(soon, nx - soon)], hx.at[:, pl.ds(soon, nx - soon)]), (hy_hbm, hy), (coupling_hbm, coupling), (sym_x_hbm, sym_x),
            (sym_y_hbm, sym_y), (sym_z_hbm, sym_z),
        ))
    ]
    per = fields // tiles
    load_v = [
        [
            pltpu.make_async_copy(v_hbm.at[pl.ds(t * per, per), y], vbuf.at[y, pl.ds(t * per, per)], vsem.at[t, y])
            for y in range(ny)
        ]
        for t in range(tiles)
    ]
    loads[0].start()
    for copy in load_v[0] + load_v[1] + loads[1:2]:
        copy.start()

    along_y = [lax.rem(me // 8 + i, 4) * 8 for i in range(4)]
    along_x = [lax.rem(me // 2 + i, 4) * 2 for i in range(4)]
    cores = [lax.rem(me + i, 2) for i in range(2)]
    steps = [(a, b, c) for a in range(4) for b in range(4) for c in range(2)][1:]
    others = [along_y[a] + along_x[b] + cores[c] for a, b, c in steps]
    hops = [min(a, 4 - a) + min(b, 4 - b) for a, b, c in steps]
    farthest = [others[k] for k in sorted(range(len(steps)), key=lambda k: -hops[k])]
    above = [lax.rem(deep + i, nd) for i in (1, 2, 3)]

    barrier = pltpu.get_barrier_semaphore()
    for peer in farthest:
        pl.semaphore_signal(
            barrier, inc=1, device_id={"north": peer, "deep": deep}, device_id_type=MESH
        )
    for peer in above:
        pl.semaphore_signal(
            barrier, inc=1, device_id={"north": me, "deep": peer}, device_id_type=MESH
        )

    def transform_x(y, first, last, high, low, begin):
        span = nn * rows
        pick = pl.ds(first * span, (last - first) * span)
        result = product(hx[0, pick, :], hx[1, pick, :], high, low, transposed=True)
        for c in range(first, last):
            part = result[(c - first) * span : (c - first + 1) * span]
            for k in range(part.shape[1] // 128):
                sbuf[c, begin + k, pl.ds(y, span, stride=ny), :] = part[:, k * 128 : (k + 1) * 128]

    def first_x(t):
        for y in range(0, ny, 2):
            load_v[t][y].wait()
            load_v[t][y + 1].wait()
            for k in (y, y + 1):
                high, low = split(vbuf[k, t * per : (t + 1) * per].reshape(128, nx))
                vhi[k, t * 128 : (t + 1) * 128] = high
                vlo[k, t * 128 : (t + 1) * 128] = low
                transform_x(k, 0, FIRST, high, low, t)

    def north(c, t, start):
        slot = c * tiles + t

        def copy(source, target, peer):
            return pltpu.make_async_remote_copy(
                src_ref=source,
                dst_ref=target,
                send_sem=ssem.at[slot],
                recv_sem=rsem.at[slot],
                device_id={"north": peer, "deep": deep},
                device_id_type=MESH,
            )

        if not start:
            everything = rbuf.at[c, t, pl.ds(0, nn - 1)]
            return copy(everything, everything, me)
        for peer in farthest:
            copy(sbuf.at[c, t, pl.ds(pl.multiple_of(peer * piece, piece), piece)], rbuf.at[c, t, me], peer).start()
        rbuf[c, t, me] = sbuf[c, t, pl.ds(pl.multiple_of(me * piece, piece), piece), :]

    def vertical(c, t, start):
        slot = c * tiles + t

        def copy(source, target, peer):
            return pltpu.make_async_remote_copy(
                src_ref=source,
                dst_ref=target,
                send_sem=dssem.at[slot],
                recv_sem=drsem.at[slot],
                device_id={"north": me, "deep": peer},
                device_id_type=MESH,
            )

        if not start:
            everything = drecv.at[c, t, pl.ds(0, nd - 1)]
            return copy(everything, everything, deep)
        for peer in above:
            copy(dsend.at[c, t, peer], drecv.at[c, t, deep], peer).start()
        drecv[c, t, deep] = dsend[c, t, deep]

    def rest_x(start, stop):
        @pl.loop(start, stop)
        def _(y):
            transform_x(y, FIRST, chunks, vhi[y], vlo[y], 0)

    def stage_y(c, t):
        north(c, t, False).wait_recv()
        for j in range(rows):
            high, low = split(rbuf[c, t, :, pl.ds(j * ny, ny), :].reshape(full_y, 128))
            result = product(hy[0], hy[1], high, low)
            for d in range(nd):
                dsend[c, t, d, j] = result[d * share_y : (d + 1) * share_y]
        vertical(c, t, True)

    def weight_of(x):
        return 1.0 / (1.0 + (sym_x[me * share_x + x] + syz[...]))

    def stage_z(c):
        for t in range(tiles):
            vertical(c, t, False).wait_recv()
        for j in range(rows):
            x = c * rows + j
            old = transform_z([[drecv[c, t, d, j] for d in range(nd)] for t in range(tiles)], hy, nz)
            for a, values in enumerate(mixed_with(old, lambda a, b: coupling[a, b], weight_of(x))):
                out[a, x] = values

    loads[0].wait()
    first_x(0)
    for copy in loads[2:]:
        copy.start()
    pl.semaphore_wait(barrier, nn - 1 + nd - 1)
    north(0, 0, True)
    first_x(1)
    north(0, 1, True)
    loads[1].wait()
    rest_x(0, 2)
    north(1, 0, True)
    north(1, 1, True)
    rest_x(2, 5)
    for copy in loads[2:]:
        copy.wait()
    stage_y(0, 0)
    north(2, 0, True)
    rest_x(5, 6)
    stage_y(0, 1)
    north(2, 1, True)
    rest_x(6, 8)
    for c in range(FIRST, AHEAD):
        for t in range(tiles):
            north(c, t, True)

    lane = lax.broadcasted_iota(jnp.int32, (share_y, full_y), 1)
    row = lax.broadcasted_iota(jnp.int32, (share_y, full_y), 0)
    mine = jnp.where(lane == row + deep * share_y, sym_y[...], 0.0)
    syz[...] = jnp.sum(mine, axis=1, keepdims=True) + sym_z[...]

    def step(c, more, ready):
        stage_y(c, 0)
        if more:
            north(c + AHEAD - 1, 0, True)
        if ready:
            stage_z(c - LAG)
        stage_y(c, 1)
        if more:
            north(c + AHEAD - 1, 1, True)

    for first, last, more, ready in (
        (1, LAG, True, False),
        (LAG, chunks - AHEAD + 1, True, True),
        (chunks - AHEAD + 1, chunks, False, True),
    ):
        @pl.loop(first, last)
        def _(c):
            step(c, more, ready)

    @pl.loop(chunks - LAG, chunks - 1)
    def _(c):
        stage_z(c)

    table[...] = hy[...]
    weight[...] = weight_of(share_x - 1)
    for a in range(fields):
        for b in range(fields):
            mixing[pl.ds(a * fields + b, 1), :] = jnp.full((1, mixing.shape[1]), coupling[a, b], F32)
    for t in range(tiles):
        vertical(chunks - 1, t, False).wait_recv()
        for d in range(nd):
            tail[t, d] = drecv[chunks - 1, t, d, 0]

    @pl.loop(0, chunks)
    def _(c):
        for t in range(tiles):
            north(c, t, False).wait_send()
            vertical(c, t, False).wait_send()


def on_device(nn, nd, velocity, coupling, symbol_x, symbol_y, symbol_z):
    fields, nx, ny, nz = velocity.shape
    share_x = nx // nn
    rows = share_x // CHUNKS
    full_y, full_z = ny * nn, nz * nd
    share_y = full_y // nd
    wide = fields * nz
    tiles = wide // 128
    order = np.arange(nx).reshape(nn, CHUNKS, rows).transpose(1, 0, 2).reshape(-1)
    table_x = jnp.asarray(two_parts(basis_table(nx)[order]))
    table_y = jnp.asarray(two_parts(basis_table(full_y)))
    dma = pltpu.SemaphoreType.DMA
    vector = pl.BlockSpec(memory_space=pltpu.VMEM)
    made = pl.pallas_call(
        functools.partial(kernel, nn, nd),
        out_shape=(
            jax.ShapeDtypeStruct((fields, share_x, share_y, full_z), F32),
            jax.ShapeDtypeStruct((tiles, nd, share_y, 128), F32),
            jax.ShapeDtypeStruct((2, full_y, full_y), BF16),
            jax.ShapeDtypeStruct((share_y, full_z), F32),
            jax.ShapeDtypeStruct((fields * fields, full_z), F32),
        ),
        in_specs=[pl.BlockSpec(memory_space=pltpu.MemorySpace.HBM)] * 7,
        out_specs=(vector,) * 5,
        scratch_shapes=[
            pltpu.VMEM((ny, fields, nz, nx), F32),
            pltpu.VMEM((ny, wide, nx), BF16),
            pltpu.VMEM((ny, wide, nx), BF16),
            pltpu.VMEM((2, nx, nx), BF16),
            pltpu.VMEM((2, full_y, full_y), BF16),
            pltpu.VMEM((CHUNKS, tiles, nn * rows * ny, 128), F32),
            pltpu.VMEM((CHUNKS, tiles, nn, rows * ny, 128), F32),
            pltpu.VMEM((CHUNKS, tiles, nd, rows, share_y, 128), F32),
            pltpu.VMEM((CHUNKS, tiles, nd, rows, share_y, 128), F32),
            pltpu.VMEM((share_y, full_z), F32),
            pltpu.SMEM((fields, fields), F32),
            pltpu.SMEM((nx,), F32),
            pltpu.VMEM((1, full_y), F32),
            pltpu.VMEM((1, full_z), F32),
            dma((tiles, ny)), dma((7,)),
            dma((CHUNKS * tiles,)), dma((CHUNKS * tiles,)), dma((CHUNKS * tiles,)), dma((CHUNKS * tiles,)),
        ],
        compiler_params=pltpu.CompilerParams(
            collective_id=0, has_side_effects=True, vmem_limit_bytes=32 << 20
        ),
    )(*(
        pltpu.with_memory_space_constraint(array, pltpu.MemorySpace.HBM)
        for array in (
            jnp.transpose(velocity, (0, 2, 3, 1)), table_x, table_y, coupling, symbol_x,
            symbol_y.reshape(1, full_y), symbol_z.reshape(1, full_z),
        )
    ))

    return pl.pallas_call(
        functools.partial(finish, nz),
        out_shape=jax.ShapeDtypeStruct((fields, share_x, share_y, full_z), F32),
        in_specs=[vector] * 5,
        out_specs=pl.BlockSpec(memory_space=pl.ANY),
        scratch_shapes=[pltpu.VMEM((fields, share_y, full_z), F32), dma((2 * fields,))],
        compiler_params=pltpu.CompilerParams(vmem_limit_bytes=8 << 20),
    )(*made)


def solution(mesh):
    placed = (P(None, None, "north", "deep"), P(), P(), P(), P())
    return jax.shard_map(
        functools.partial(on_device, mesh.shape["north"], mesh.shape["deep"]),
        mesh=mesh,
        in_specs=placed,
        out_specs=P(None, "north", "deep", None),
        check_vma=False,
    )
```

```python
import functools

import jax
import jax.numpy as jnp
import numpy as np
from jax import lax
from jax.experimental import pallas as pl
from jax.experimental.pallas import tpu as pltpu
from jax.sharding import PartitionSpec as P

MESH = pl.DeviceIdType.MESH
F32, BF16 = jnp.float32, jnp.bfloat16
CHUNKS = 16
FIRST = 3
LAG = 3
AHEAD = 4


def basis_table(count):
    rank = np.arange(1, count + 1)
    turns = (rank[:, None] * rank[None, :]) % (2 * count + 2)
    return np.sin(np.pi * turns / (count + 1)) * np.sqrt(2.0 / (count + 1))


def two_parts(table):
    high = table.astype(BF16)
    low = (table - high.astype(np.float64)).astype(BF16)
    return np.stack([high, low])


def split(values):
    high = values.astype(BF16)
    return high, (values - high.astype(F32)).astype(BF16)


def dot(a, b, transposed=False):
    dims = (((1,), (1 if transposed else 0,)), ((), ()))
    return lax.dot_general(a, b, dims, preferred_element_type=F32)


def product(a_high, a_low, b_high, b_low, transposed=False):
    count = a_high.shape[0]
    both = dot(jnp.concatenate([a_high, a_low], axis=0), b_high, transposed)
    return both[:count] + (both[count:] + dot(a_high, b_low, transposed))


def transform_z(pieces, table, nz):
    lower = lax.broadcasted_iota(jnp.int32, pieces[0][0].shape, 1) < nz
    lines = []
    for parts in pieces:
        turned = [pltpu.roll(p, nz, 1) for p in parts]
        pairs = range(0, len(parts), 2)
        even = [jnp.where(lower, parts[d], turned[d + 1]) for d in pairs]
        odd = [jnp.where(lower, turned[d], parts[d + 1]) for d in pairs]
        lines.append(jnp.concatenate(even, axis=1))
        lines.append(jnp.concatenate(odd, axis=1))
    high, low = split(jnp.concatenate(lines, axis=0))
    result = product(high, low, table[0], table[1])
    share = pieces[0][0].shape[0]
    return [result[f * share : (f + 1) * share] for f in range(len(lines))]


def mixed_with(old, coupling, weight):
    rest = 1.0 - weight
    for a in range(len(old)):
        mixed = coupling(a, 0) * old[0]
        for b in range(1, len(old)):
            mixed = mixed + coupling(a, b) * old[b]
        yield weight * old[a] + rest * mixed


def finish(nz, most, last, table, weight, coupling, result, final, sem):
    fields, share_x = most.shape[:2]
    copies = [
        pltpu.make_async_copy(most.at[f, pl.ds(0, share_x - 1)], result.at[f, pl.ds(0, share_x - 1)], sem.at[f])
        for f in range(fields)
    ]
    for copy in copies:
        copy.start()
    tiles, nd = last.shape[:2]
    old = transform_z([[last[t, d] for d in range(nd)] for t in range(tiles)], table, nz)

    def factor(a, b):
        return coupling[pl.ds(a * fields + b, 1), :]

    for a, values in enumerate(mixed_with(old, factor, weight[...])):
        final[a] = values
        copies.append(pltpu.make_async_copy(final.at[a], result.at[a, share_x - 1], sem.at[fields + a]))
        copies[-1].start()
    for copy in copies:
        copy.wait()


def kernel(
    nn, nd, v_hbm, hx_hbm, hy_hbm, coupling_hbm, sym_x_hbm, sym_y_hbm, sym_z_hbm, out, tail, table, weight, mixing,
    vbuf, vhi, vlo, hx, hy, sbuf, rbuf, dsend, drecv, syz, coupling, sym_x, sym_y, sym_z,
    vsem, hsem, ssem, rsem, dssem, drsem,
):
    fields, ny, nz, nx = v_hbm.shape
    chunks = sbuf.shape[0]
    share_x = nx // nn
    rows = share_x // chunks
    wide = fields * nz
    tiles = wide // 128
    full_y = nn * ny
    share_y = full_y // nd
    piece = rows * ny
    me, deep = lax.axis_index("north"), lax.axis_index("deep")

    soon = FIRST * nn * rows
    loads = [
        pltpu.make_async_copy(a, b, hsem.at[k])
        for k, (a, b) in enumerate((
            (hx_hbm.at[:, pl.ds(0, soon)], hx.at[:, pl.ds(0, soon)]),
            (hx_hbm.at[:, pl.ds(soon, nx - soon)], hx.at[:, pl.ds(soon, nx - soon)]), (hy_hbm, hy), (coupling_hbm, coupling), (sym_x_hbm, sym_x),
            (sym_y_hbm, sym_y), (sym_z_hbm, sym_z),
        ))
    ]
    per = fields // tiles
    load_v = [
        [
            pltpu.make_async_copy(
                v_hbm.at[pl.ds(t * per, per), pl.ds(y, 2)], vbuf.at[pl.ds(t * per, per), pl.ds(y, 2)], vsem.at[t, y // 2]
            )
            for y in range(0, ny, 2)
        ]
        for t in range(tiles)
    ]
    loads[0].start()
    for copy in load_v[0] + load_v[1] + loads[1:2]:
        copy.start()

    along_y = [lax.rem(me // 8 + i, 4) * 8 for i in range(4)]
    along_x = [lax.rem(me // 2 + i, 4) * 2 for i in range(4)]
    cores = [lax.rem(me + i, 2) for i in range(2)]
    steps = [(a, b, c) for a in range(4) for b in range(4) for c in range(2)][1:]
    others = [along_y[a] + along_x[b] + cores[c] for a, b, c in steps]
    hops = [min(a, 4 - a) + min(b, 4 - b) for a, b, c in steps]
    farthest = [others[k] for k in sorted(range(len(steps)), key=lambda k: -hops[k])]
    above = [lax.rem(deep + i, nd) for i in (1, 2, 3)]

    barrier = pltpu.get_barrier_semaphore()
    for peer in farthest:
        pl.semaphore_signal(
            barrier, inc=1, device_id={"north": peer, "deep": deep}, device_id_type=MESH
        )
    for peer in above:
        pl.semaphore_signal(
            barrier, inc=1, device_id={"north": me, "deep": peer}, device_id_type=MESH
        )

    def transform_x(y, first, last, high, low, begin):
        span = nn * rows
        pick = pl.ds(first * span, (last - first) * span)
        result = product(hx[0, pick, :], hx[1, pick, :], high, low, transposed=True)
        for c in range(first, last):
            part = result[(c - first) * span : (c - first + 1) * span]
            for k in range(part.shape[1] // 128):
                sbuf[c, begin + k, pl.ds(y, span, stride=ny), :] = part[:, k * 128 : (k + 1) * 128]

    def first_x(t):
        for y in range(0, ny, 2):
            load_v[t][y // 2].wait()
            for k in (y, y + 1):
                high, low = split(vbuf[t * per : (t + 1) * per, k].reshape(128, nx))
                vhi[k, t * 128 : (t + 1) * 128] = high
                vlo[k, t * 128 : (t + 1) * 128] = low
                transform_x(k, 0, FIRST, high, low, t)

    def north(c, t, start):
        slot = c * tiles + t

        def copy(source, target, peer):
            return pltpu.make_async_remote_copy(
                src_ref=source,
                dst_ref=target,
                send_sem=ssem.at[0],
                recv_sem=rsem.at[slot],
                device_id={"north": peer, "deep": deep},
                device_id_type=MESH,
            )

        if not start:
            everything = rbuf.at[c, t, pl.ds(0, nn - 1)]
            return copy(everything, everything, me)
        for peer in farthest:
            copy(sbuf.at[c, t, pl.ds(pl.multiple_of(peer * piece, piece), piece)], rbuf.at[c, t, me], peer).start()
        rbuf[c, t, me] = sbuf[c, t, pl.ds(pl.multiple_of(me * piece, piece), piece), :]

    def vertical(c, t, start):
        slot = c * tiles + t

        def copy(source, target, peer):
            return pltpu.make_async_remote_copy(
                src_ref=source,
                dst_ref=target,
                send_sem=dssem.at[0],
                recv_sem=drsem.at[slot],
                device_id={"north": me, "deep": peer},
                device_id_type=MESH,
            )

        if not start:
            everything = drecv.at[c, t, pl.ds(0, nd - 1)]
            return copy(everything, everything, deep)
        for peer in above:
            copy(dsend.at[c, t, peer], drecv.at[c, t, deep], peer).start()
        drecv[c, t, deep] = dsend[c, t, deep]

    def rest_x(start, stop):
        @pl.loop(start, stop)
        def _(y):
            transform_x(y, FIRST, chunks, vhi[y], vlo[y], 0)

    def stage_y(c, t):
        north(c, t, False).wait_recv()
        for j in range(rows):
            high, low = split(rbuf[c, t, :, pl.ds(j * ny, ny), :].reshape(full_y, 128))
            result = product(hy[0], hy[1], high, low)
            for d in range(nd):
                dsend[c, t, d, j] = result[d * share_y : (d + 1) * share_y]
        vertical(c, t, True)

    def weight_of(x):
        return 1.0 / (1.0 + (sym_x[me * share_x + x] + syz[...]))

    def stage_z(c):
        for t in range(tiles):
            vertical(c, t, False).wait_recv()
        for j in range(rows):
            x = c * rows + j
            old = transform_z([[drecv[c, t, d, j] for d in range(nd)] for t in range(tiles)], hy, nz)
            for a, values in enumerate(mixed_with(old, lambda a, b: coupling[a, b], weight_of(x))):
                out[a, x] = values

    loads[0].wait()
    first_x(0)
    for copy in loads[2:]:
        copy.start()
    pl.semaphore_wait(barrier, nn - 1 + nd - 1)
    north(0, 0, True)
    first_x(1)
    north(0, 1, True)
    loads[1].wait()
    rest_x(0, 2)
    north(1, 0, True)
    north(1, 1, True)
    rest_x(2, 5)
    for copy in loads[2:]:
        copy.wait()
    stage_y(0, 0)
    north(2, 0, True)
    rest_x(5, 6)
    stage_y(0, 1)
    north(2, 1, True)
    rest_x(6, 8)
    for c in range(FIRST, AHEAD):
        for t in range(tiles):
            north(c, t, True)

    lane = lax.broadcasted_iota(jnp.int32, (share_y, full_y), 1)
    row = lax.broadcasted_iota(jnp.int32, (share_y, full_y), 0)
    mine = jnp.where(lane == row + deep * share_y, sym_y[...], 0.0)
    syz[...] = jnp.sum(mine, axis=1, keepdims=True) + sym_z[...]

    def step(c, more, ready):
        stage_y(c, 0)
        if more:
            north(c + AHEAD - 1, 0, True)
        if ready:
            stage_z(c - LAG)
        stage_y(c, 1)
        if more:
            north(c + AHEAD - 1, 1, True)

    for first, last, more, ready in (
        (1, LAG, True, False),
        (LAG, chunks - AHEAD + 1, True, True),
        (chunks - AHEAD + 1, chunks, False, True),
    ):
        @pl.loop(first, last)
        def _(c):
            step(c, more, ready)

    @pl.loop(chunks - LAG, chunks - 1)
    def _(c):
        stage_z(c)

    table[...] = hy[...]
    weight[...] = weight_of(share_x - 1)
    for a in range(fields):
        for b in range(fields):
            mixing[pl.ds(a * fields + b, 1), :] = jnp.full((1, mixing.shape[1]), coupling[a, b], F32)
    for t in range(tiles):
        vertical(chunks - 1, t, False).wait_recv()
        for d in range(nd):
            tail[t, d] = drecv[chunks - 1, t, d, 0]

    for buffer, count, sent, received in ((rbuf, nn - 1, ssem, rsem), (drecv, nd - 1, dssem, drsem)):
        everything = buffer.at[:, :, pl.ds(0, count)]
        pltpu.make_async_remote_copy(
            src_ref=everything,
            dst_ref=everything,
            send_sem=sent.at[0],
            recv_sem=received.at[0],
            device_id={"north": me, "deep": deep},
            device_id_type=MESH,
        ).wait_send()


def on_device(nn, nd, velocity, coupling, symbol_x, symbol_y, symbol_z):
    fields, nx, ny, nz = velocity.shape
    share_x = nx // nn
    rows = share_x // CHUNKS
    full_y, full_z = ny * nn, nz * nd
    share_y = full_y // nd
    wide = fields * nz
    tiles = wide // 128
    order = np.arange(nx).reshape(nn, CHUNKS, rows).transpose(1, 0, 2).reshape(-1)
    table_x = jnp.asarray(two_parts(basis_table(nx)[order]))
    table_y = jnp.asarray(two_parts(basis_table(full_y)))
    dma = pltpu.SemaphoreType.DMA
    vector = pl.BlockSpec(memory_space=pltpu.VMEM)
    made = pl.pallas_call(
        functools.partial(kernel, nn, nd),
        out_shape=(
            jax.ShapeDtypeStruct((fields, share_x, share_y, full_z), F32),
            jax.ShapeDtypeStruct((tiles, nd, share_y, 128), F32),
            jax.ShapeDtypeStruct((2, full_y, full_y), BF16),
            jax.ShapeDtypeStruct((share_y, full_z), F32),
            jax.ShapeDtypeStruct((fields * fields, full_z), F32),
        ),
        in_specs=[pl.BlockSpec(memory_space=pltpu.MemorySpace.HBM)] * 7,
        out_specs=(vector,) * 5,
        scratch_shapes=[
            pltpu.VMEM((fields, ny, nz, nx), F32),
            pltpu.VMEM((ny, wide, nx), BF16),
            pltpu.VMEM((ny, wide, nx), BF16),
            pltpu.VMEM((2, nx, nx), BF16),
            pltpu.VMEM((2, full_y, full_y), BF16),
            pltpu.VMEM((CHUNKS, tiles, nn * rows * ny, 128), F32),
            pltpu.VMEM((CHUNKS, tiles, nn, rows * ny, 128), F32),
            pltpu.VMEM((CHUNKS, tiles, nd, rows, share_y, 128), F32),
            pltpu.VMEM((CHUNKS, tiles, nd, rows, share_y, 128), F32),
            pltpu.VMEM((share_y, full_z), F32),
            pltpu.SMEM((fields, fields), F32),
            pltpu.SMEM((nx,), F32),
            pltpu.VMEM((1, full_y), F32),
            pltpu.VMEM((1, full_z), F32),
            dma((tiles, ny // 2)), dma((7,)),
            dma((1,)), dma((CHUNKS * tiles,)), dma((1,)), dma((CHUNKS * tiles,)),
        ],
        compiler_params=pltpu.CompilerParams(
            collective_id=0, has_side_effects=True, vmem_limit_bytes=32 << 20
        ),
    )(*(
        pltpu.with_memory_space_constraint(array, pltpu.MemorySpace.HBM)
        for array in (
            jnp.transpose(velocity, (0, 2, 3, 1)), table_x, table_y, coupling, symbol_x,
            symbol_y.reshape(1, full_y), symbol_z.reshape(1, full_z),
        )
    ))

    return pl.pallas_call(
        functools.partial(finish, nz),
        out_shape=jax.ShapeDtypeStruct((fields, share_x, share_y, full_z), F32),
        in_specs=[vector] * 5,
        out_specs=pl.BlockSpec(memory_space=pl.ANY),
        scratch_shapes=[pltpu.VMEM((fields, share_y, full_z), F32), dma((2 * fields,))],
        compiler_params=pltpu.CompilerParams(vmem_limit_bytes=8 << 20),
    )(*made)


def solution(mesh):
    placed = (P(None, None, "north", "deep"), P(), P(), P(), P())
    return jax.shard_map(
        functools.partial(on_device, mesh.shape["north"], mesh.shape["deep"]),
        mesh=mesh,
        in_specs=placed,
        out_specs=P(None, "north", "deep", None),
        check_vma=False,
    )
```

```python
import functools

import jax
import jax.numpy as jnp
import numpy as np
from jax import lax
from jax.experimental import pallas as pl
from jax.experimental.pallas import tpu as pltpu
from jax.sharding import PartitionSpec as P

MESH = pl.DeviceIdType.MESH
F32, BF16 = jnp.float32, jnp.bfloat16
CHUNKS = 16
FIRST = 3
LAG = 3
AHEAD = 4
CYCLE = 8


def basis_table(count):
    rank = np.arange(1, count + 1)
    turns = (rank[:, None] * rank[None, :]) % (2 * count + 2)
    return np.sin(np.pi * turns / (count + 1)) * np.sqrt(2.0 / (count + 1))


def two_parts(table):
    high = table.astype(BF16)
    low = (table - high.astype(np.float64)).astype(BF16)
    return np.stack([high, low])


def split(values):
    high = values.astype(BF16)
    return high, (values - high.astype(F32)).astype(BF16)


def dot(a, b, transposed=False):
    dims = (((1,), (1 if transposed else 0,)), ((), ()))
    return lax.dot_general(a, b, dims, preferred_element_type=F32)


def product(a_high, a_low, b_high, b_low, transposed=False):
    count = a_high.shape[0]
    both = dot(jnp.concatenate([a_high, a_low], axis=0), b_high, transposed)
    return both[:count] + (both[count:] + dot(a_high, b_low, transposed))


def transform_z(pieces, table, nz):
    lower = lax.broadcasted_iota(jnp.int32, pieces[0][0].shape, 1) < nz
    lines = []
    for parts in pieces:
        turned = [pltpu.roll(p, nz, 1) for p in parts]
        pairs = range(0, len(parts), 2)
        even = [jnp.where(lower, parts[d], turned[d + 1]) for d in pairs]
        odd = [jnp.where(lower, turned[d], parts[d + 1]) for d in pairs]
        lines.append(jnp.concatenate(even, axis=1))
        lines.append(jnp.concatenate(odd, axis=1))
    high, low = split(jnp.concatenate(lines, axis=0))
    result = product(high, low, table[0], table[1])
    share = pieces[0][0].shape[0]
    return [result[f * share : (f + 1) * share] for f in range(len(lines))]


def mixed_with(old, coupling, weight):
    rest = 1.0 - weight
    for a in range(len(old)):
        mixed = coupling(a, 0) * old[0]
        for b in range(1, len(old)):
            mixed = mixed + coupling(a, b) * old[b]
        yield weight * old[a] + rest * mixed


def finish(nz, most, last, table, weight, coupling, result, final, sem):
    fields, share_x = most.shape[:2]
    copies = [
        pltpu.make_async_copy(most.at[f, pl.ds(0, share_x - 1)], result.at[f, pl.ds(0, share_x - 1)], sem.at[f])
        for f in range(fields)
    ]
    for copy in copies:
        copy.start()
    tiles, nd = last.shape[:2]
    old = transform_z([[last[t, d] for d in range(nd)] for t in range(tiles)], table, nz)

    def factor(a, b):
        return coupling[pl.ds(a * fields + b, 1), :]

    for a, values in enumerate(mixed_with(old, factor, weight[...])):
        final[a] = values
        copies.append(pltpu.make_async_copy(final.at[a], result.at[a, share_x - 1], sem.at[fields + a]))
        copies[-1].start()
    for copy in copies:
        copy.wait()


def kernel(
    nn, nd, v_hbm, hx_hbm, hy_hbm, coupling_hbm, sym_x_hbm, sym_y_hbm, sym_z_hbm, out, tail, table, weight, mixing,
    vbuf, vhi, vlo, hx, hy, sbuf, rbuf, dsend, drecv, syz, coupling, sym_x, sym_y, sym_z,
    vsem, hsem, ssem, rsem, dssem, drsem,
):
    fields, ny, nz, nx = v_hbm.shape
    chunks = sbuf.shape[0]
    share_x = nx // nn
    rows = share_x // chunks
    wide = fields * nz
    tiles = wide // 128
    full_y = nn * ny
    share_y = full_y // nd
    piece = rows * ny
    me, deep = lax.axis_index("north"), lax.axis_index("deep")

    soon = FIRST * nn * rows
    loads = [
        pltpu.make_async_copy(a, b, hsem.at[k])
        for k, (a, b) in enumerate((
            (hx_hbm.at[:, pl.ds(0, soon)], hx.at[:, pl.ds(0, soon)]),
            (hx_hbm.at[:, pl.ds(soon, nx - soon)], hx.at[:, pl.ds(soon, nx - soon)]), (hy_hbm, hy), (coupling_hbm, coupling), (sym_x_hbm, sym_x),
            (sym_y_hbm, sym_y), (sym_z_hbm, sym_z),
        ))
    ]
    per = fields // tiles
    load_v = [
        [
            pltpu.make_async_copy(
                v_hbm.at[pl.ds(t * per, per), pl.ds(y, 2)], vbuf.at[pl.ds(t * per, per), pl.ds(y, 2)], vsem.at[t, y // 2]
            )
            for y in range(0, ny, 2)
        ]
        for t in range(tiles)
    ]
    loads[0].start()
    for copy in load_v[0]:
        copy.start()

    along_y = [lax.rem(me // 8 + i, 4) * 8 for i in range(4)]
    along_x = [lax.rem(me // 2 + i, 4) * 2 for i in range(4)]
    cores = [lax.rem(me + i, 2) for i in range(2)]
    steps = [(a, b, c) for a in range(4) for b in range(4) for c in range(2)][1:]
    others = [along_y[a] + along_x[b] + cores[c] for a, b, c in steps]
    hops = [min(a, 4 - a) + min(b, 4 - b) for a, b, c in steps]
    farthest = [others[k] for k in sorted(range(len(steps)), key=lambda k: -hops[k])]
    above = [k + lax.div(k + nd - deep, nd) for k in range(nd - 1)]

    barrier = pltpu.get_barrier_semaphore()
    for peer in farthest:
        pl.semaphore_signal(
            barrier, inc=1, device_id={"north": peer, "deep": deep}, device_id_type=MESH
        )
    for peer in above:
        pl.semaphore_signal(
            barrier, inc=1, device_id={"north": me, "deep": peer}, device_id_type=MESH
        )

    for copy in load_v[1] + loads[1:2]:
        copy.start()

    def transform_x(y, first, last, high, low, begin):
        span = nn * rows
        pick = pl.ds(first * span, (last - first) * span)
        result = product(hx[0, pick, :], hx[1, pick, :], high, low, transposed=True)
        for c in range(first, last):
            part = result[(c - first) * span : (c - first + 1) * span]
            for k in range(part.shape[1] // 128):
                sbuf[c, begin + k, pl.ds(y, span, stride=ny), :] = part[:, k * 128 : (k + 1) * 128]

    def first_x(t):
        for y in range(0, ny, 2):
            load_v[t][y // 2].wait()
            for k in (y, y + 1):
                high, low = split(vbuf[t * per : (t + 1) * per, k].reshape(128, nx))
                vhi[k, t * 128 : (t + 1) * 128] = high
                vlo[k, t * 128 : (t + 1) * 128] = low
                transform_x(k, 0, FIRST, high, low, t)

    def north(c, t, start):
        slot = c % CYCLE * tiles + t if isinstance(c, int) else lax.rem(c, CYCLE) * tiles + t

        def copy(source, target, peer):
            return pltpu.make_async_remote_copy(
                src_ref=source,
                dst_ref=target,
                send_sem=ssem.at[0],
                recv_sem=rsem.at[slot],
                device_id={"north": peer, "deep": deep},
                device_id_type=MESH,
            )

        if not start:
            everything = rbuf.at[c, t, pl.ds(0, nn - 1)]
            return copy(everything, everything, me)
        for peer in farthest:
            copy(sbuf.at[c, t, pl.ds(pl.multiple_of(peer * piece, piece), piece)], rbuf.at[c, t, me], peer).start()
        rbuf[c, t, me] = sbuf[c, t, pl.ds(pl.multiple_of(me * piece, piece), piece), :]

    def vertical(c, t, start):
        slot = c % CYCLE * tiles + t if isinstance(c, int) else lax.rem(c, CYCLE) * tiles + t

        def copy(source, target, peer):
            return pltpu.make_async_remote_copy(
                src_ref=source,
                dst_ref=target,
                send_sem=dssem.at[0],
                recv_sem=drsem.at[slot],
                device_id={"north": me, "deep": peer},
                device_id_type=MESH,
            )

        if not start:
            everything = drecv.at[c, t, pl.ds(0, nd - 1)]
            return copy(everything, everything, deep)
        for peer in above:
            copy(dsend.at[c, t, peer], drecv.at[c, t, deep], peer).start()
        drecv[c, t, deep] = dsend[c, t, deep]

    def rest_x(start, stop):
        @pl.loop(start, stop)
        def _(y):
            transform_x(y, FIRST, chunks, vhi[y], vlo[y], 0)

    def stage_y(c, t):
        north(c, t, False).wait_recv()
        for j in range(rows):
            high, low = split(rbuf[c, t, :, pl.ds(j * ny, ny), :].reshape(full_y, 128))
            result = product(hy[0], hy[1], high, low)
            for d in range(nd):
                dsend[c, t, d, j] = result[d * share_y : (d + 1) * share_y]
        vertical(c, t, True)

    def weight_of(x):
        return 1.0 / (1.0 + (sym_x[me * share_x + x] + syz[...]))

    def stage_z(c):
        for t in range(tiles):
            vertical(c, t, False).wait_recv()
        for j in range(rows):
            x = c * rows + j
            old = transform_z([[drecv[c, t, d, j] for d in range(nd)] for t in range(tiles)], hy, nz)
            for a, values in enumerate(mixed_with(old, lambda a, b: coupling[a, b], weight_of(x))):
                out[a, x] = values

    loads[0].wait()
    first_x(0)
    for copy in loads[2:]:
        copy.start()
    pl.semaphore_wait(barrier, nn - 1 + nd - 1)
    north(0, 0, True)
    first_x(1)
    north(0, 1, True)
    loads[1].wait()
    rest_x(0, 2)
    north(1, 0, True)
    north(1, 1, True)
    rest_x(2, 5)
    for copy in loads[2:]:
        copy.wait()
    stage_y(0, 0)
    north(2, 0, True)
    rest_x(5, 6)
    stage_y(0, 1)
    north(2, 1, True)
    rest_x(6, 8)
    for c in range(FIRST, AHEAD):
        for t in range(tiles):
            north(c, t, True)

    lane = lax.broadcasted_iota(jnp.int32, (share_y, full_y), 1)
    row = lax.broadcasted_iota(jnp.int32, (share_y, full_y), 0)
    mine = jnp.where(lane == row + deep * share_y, sym_y[...], 0.0)
    syz[...] = jnp.sum(mine, axis=1, keepdims=True) + sym_z[...]

    def step(c, more, ready):
        stage_y(c, 0)
        if more:
            north(c + AHEAD - 1, 0, True)
        if ready:
            stage_z(c - LAG)
        stage_y(c, 1)
        if more:
            north(c + AHEAD - 1, 1, True)

    for first, last, more, ready in (
        (1, LAG, True, False),
        (LAG, chunks - AHEAD + 1, True, True),
        (chunks - AHEAD + 1, chunks, False, True),
    ):
        @pl.loop(first, last)
        def _(c):
            step(c, more, ready)

    @pl.loop(chunks - LAG, chunks - 1)
    def _(c):
        stage_z(c)

    table[...] = hy[...]
    weight[...] = weight_of(share_x - 1)
    for a in range(fields):
        for b in range(fields):
            mixing[pl.ds(a * fields + b, 1), :] = jnp.full((1, mixing.shape[1]), coupling[a, b], F32)
    for t in range(tiles):
        vertical(chunks - 1, t, False).wait_recv()
        for d in range(nd):
            tail[t, d] = drecv[chunks - 1, t, d, 0]

    for buffer, count, sent, received in ((rbuf, nn - 1, ssem, rsem), (drecv, nd - 1, dssem, drsem)):
        everything = buffer.at[:, :, pl.ds(0, count)]
        pltpu.make_async_remote_copy(
            src_ref=everything,
            dst_ref=everything,
            send_sem=sent.at[0],
            recv_sem=received.at[0],
            device_id={"north": me, "deep": deep},
            device_id_type=MESH,
        ).wait_send()


def on_device(nn, nd, velocity, coupling, symbol_x, symbol_y, symbol_z):
    fields, nx, ny, nz = velocity.shape
    share_x = nx // nn
    rows = share_x // CHUNKS
    full_y, full_z = ny * nn, nz * nd
    share_y = full_y // nd
    wide = fields * nz
    tiles = wide // 128
    order = np.arange(nx).reshape(nn, CHUNKS, rows).transpose(1, 0, 2).reshape(-1)
    table_x = jnp.asarray(two_parts(basis_table(nx)[order]))
    table_y = jnp.asarray(two_parts(basis_table(full_y)))
    dma = pltpu.SemaphoreType.DMA
    vector = pl.BlockSpec(memory_space=pltpu.VMEM)
    made = pl.pallas_call(
        functools.partial(kernel, nn, nd),
        out_shape=(
            jax.ShapeDtypeStruct((fields, share_x, share_y, full_z), F32),
            jax.ShapeDtypeStruct((tiles, nd, share_y, 128), F32),
            jax.ShapeDtypeStruct((2, full_y, full_y), BF16),
            jax.ShapeDtypeStruct((share_y, full_z), F32),
            jax.ShapeDtypeStruct((fields * fields, full_z), F32),
        ),
        in_specs=[pl.BlockSpec(memory_space=pltpu.MemorySpace.HBM)] * 7,
        out_specs=(vector,) * 5,
        scratch_shapes=[
            pltpu.VMEM((fields, ny, nz, nx), F32),
            pltpu.VMEM((ny, wide, nx), BF16),
            pltpu.VMEM((ny, wide, nx), BF16),
            pltpu.VMEM((2, nx, nx), BF16),
            pltpu.VMEM((2, full_y, full_y), BF16),
            pltpu.VMEM((CHUNKS, tiles, nn * rows * ny, 128), F32),
            pltpu.VMEM((CHUNKS, tiles, nn, rows * ny, 128), F32),
            pltpu.VMEM((CHUNKS, tiles, nd, rows, share_y, 128), F32),
            pltpu.VMEM((CHUNKS, tiles, nd, rows, share_y, 128), F32),
            pltpu.VMEM((share_y, full_z), F32),
            pltpu.SMEM((fields, fields), F32),
            pltpu.SMEM((nx,), F32),
            pltpu.VMEM((1, full_y), F32),
            pltpu.VMEM((1, full_z), F32),
            dma((tiles, ny // 2)), dma((7,)),
            dma((1,)), dma((CYCLE * tiles,)), dma((1,)), dma((CYCLE * tiles,)),
        ],
        compiler_params=pltpu.CompilerParams(
            collective_id=0, has_side_effects=True, vmem_limit_bytes=32 << 20
        ),
    )(*(
        pltpu.with_memory_space_constraint(array, pltpu.MemorySpace.HBM)
        for array in (
            jnp.transpose(velocity, (0, 2, 3, 1)), table_x, table_y, coupling, symbol_x,
            symbol_y.reshape(1, full_y), symbol_z.reshape(1, full_z),
        )
    ))

    return pl.pallas_call(
        functools.partial(finish, nz),
        out_shape=jax.ShapeDtypeStruct((fields, share_x, share_y, full_z), F32),
        in_specs=[vector] * 5,
        out_specs=pl.BlockSpec(memory_space=pl.ANY),
        scratch_shapes=[pltpu.VMEM((fields, share_y, full_z), F32), dma((2 * fields,))],
        compiler_params=pltpu.CompilerParams(vmem_limit_bytes=8 << 20),
    )(*made)


def solution(mesh):
    placed = (P(None, None, "north", "deep"), P(), P(), P(), P())
    return jax.shard_map(
        functools.partial(on_device, mesh.shape["north"], mesh.shape["deep"]),
        mesh=mesh,
        in_specs=placed,
        out_specs=P(None, "north", "deep", None),
        check_vma=False,
    )
```

```python
import functools

import jax
import jax.numpy as jnp
import numpy as np
from jax import lax
from jax.experimental import pallas as pl
from jax.experimental.pallas import tpu as pltpu
from jax.sharding import PartitionSpec as P

MESH = pl.DeviceIdType.MESH
F32, BF16 = jnp.float32, jnp.bfloat16
CHUNKS = 16
FIRST = 3
LAG = 3
AHEAD = 4
CYCLE = 8


def basis_table(count):
    rank = np.arange(1, count + 1)
    turns = (rank[:, None] * rank[None, :]) % (2 * count + 2)
    return np.sin(np.pi * turns / (count + 1)) * np.sqrt(2.0 / (count + 1))


def two_parts(table):
    high = table.astype(BF16)
    low = (table - high.astype(np.float64)).astype(BF16)
    return np.stack([high, low])


def split(values):
    high = values.astype(BF16)
    return high, (values - high.astype(F32)).astype(BF16)


def dot(a, b, transposed=False):
    dims = (((1,), (1 if transposed else 0,)), ((), ()))
    return lax.dot_general(a, b, dims, preferred_element_type=F32)


def product(a_high, a_low, b_high, b_low, transposed=False):
    count = a_high.shape[0]
    both = dot(jnp.concatenate([a_high, a_low], axis=0), b_high, transposed)
    return both[:count] + (both[count:] + dot(a_high, b_low, transposed))


def transform_z(pieces, table, nz):
    lower = lax.broadcasted_iota(jnp.int32, pieces[0][0].shape, 1) < nz
    lines = []
    for parts in pieces:
        turned = [pltpu.roll(p, nz, 1) for p in parts]
        pairs = range(0, len(parts), 2)
        even = [jnp.where(lower, parts[d], turned[d + 1]) for d in pairs]
        odd = [jnp.where(lower, turned[d], parts[d + 1]) for d in pairs]
        lines.append(jnp.concatenate(even, axis=1))
        lines.append(jnp.concatenate(odd, axis=1))
    high, low = split(jnp.concatenate(lines, axis=0))
    result = product(high, low, table[0], table[1])
    share = pieces[0][0].shape[0]
    return [result[f * share : (f + 1) * share] for f in range(len(lines))]


def mixed_with(old, coupling, weight):
    rest = 1.0 - weight
    for a in range(len(old)):
        mixed = coupling(a, 0) * old[0]
        for b in range(1, len(old)):
            mixed = mixed + coupling(a, b) * old[b]
        yield weight * old[a] + rest * mixed


def finish(nz, most, last, table, weight, coupling, result, final, sem):
    fields, share_x = most.shape[:2]
    copies = [
        pltpu.make_async_copy(most.at[f, pl.ds(0, share_x - 1)], result.at[f, pl.ds(0, share_x - 1)], sem.at[f])
        for f in range(fields)
    ]
    for copy in copies:
        copy.start()
    tiles, nd = last.shape[:2]
    old = transform_z([[last[t, d] for d in range(nd)] for t in range(tiles)], table, nz)

    def factor(a, b):
        return coupling[pl.ds(a * fields + b, 1), :]

    for a, values in enumerate(mixed_with(old, factor, weight[...])):
        final[a] = values
        copies.append(pltpu.make_async_copy(final.at[a], result.at[a, share_x - 1], sem.at[fields + a]))
        copies[-1].start()
    for copy in copies:
        copy.wait()


def kernel(
    nn, nd, v_hbm, hx_hbm, hy_hbm, coupling_hbm, sym_x_hbm, sym_y_hbm, sym_z_hbm, out, tail, table, weight, mixing,
    vbuf, vhi, vlo, hx, hy, sbuf, rbuf, dsend, drecv, syz, coupling, sym_x, sym_y, sym_z,
    vsem, hsem, ssem, rsem, dssem, drsem,
):
    fields, ny, nz, nx = v_hbm.shape
    chunks = sbuf.shape[0]
    share_x = nx // nn
    rows = share_x // chunks
    wide = fields * nz
    tiles = wide // 128
    full_y = nn * ny
    share_y = full_y // nd
    piece = rows * ny
    me, deep = lax.axis_index("north"), lax.axis_index("deep")

    soon = FIRST * nn * rows
    loads = [
        pltpu.make_async_copy(a, b, hsem.at[k])
        for k, (a, b) in enumerate((
            (hx_hbm.at[:, pl.ds(0, soon)], hx.at[:, pl.ds(0, soon)]),
            (hx_hbm.at[:, pl.ds(soon, nx - soon)], hx.at[:, pl.ds(soon, nx - soon)]), (hy_hbm, hy), (coupling_hbm, coupling), (sym_x_hbm, sym_x),
            (sym_y_hbm, sym_y), (sym_z_hbm, sym_z),
        ))
    ]
    per = fields // tiles
    load_v = [
        [
            pltpu.make_async_copy(
                v_hbm.at[pl.ds(t * per, per), pl.ds(y, 2)], vbuf.at[pl.ds(t * per, per), pl.ds(y, 2)], vsem.at[t, y // 2]
            )
            for y in range(0, ny, 2)
        ]
        for t in range(tiles)
    ]
    loads[0].start()
    for copy in load_v[0]:
        copy.start()

    along_y = [lax.rem(me // 8 + i, 4) * 8 for i in range(4)]
    along_x = [lax.rem(me // 2 + i, 4) * 2 for i in range(4)]
    cores = [lax.rem(me + i, 2) for i in range(2)]
    steps = [(a, b, c) for a in range(4) for b in range(4) for c in range(2)][1:]
    others = [along_y[a] + along_x[b] + cores[c] for a, b, c in steps]
    hops = [min(a, 4 - a) + min(b, 4 - b) for a, b, c in steps]
    farthest = [others[k] for k in sorted(range(len(steps)), key=lambda k: -hops[k])]
    above = [k + lax.div(k + nd - deep, nd) for k in range(nd - 1)]

    barrier = pltpu.get_barrier_semaphore()
    for peer in farthest:
        pl.semaphore_signal(
            barrier, inc=1, device_id={"north": peer, "deep": deep}, device_id_type=MESH
        )
    for peer in above:
        pl.semaphore_signal(
            barrier, inc=1, device_id={"north": me, "deep": peer}, device_id_type=MESH
        )

    for copy in load_v[1] + loads[1:2]:
        copy.start()

    def transform_x(y, first, last, high, low, begin):
        span = nn * rows
        pick = pl.ds(first * span, (last - first) * span)
        result = product(hx[0, pick, :], hx[1, pick, :], high, low, transposed=True)
        for c in range(first, last):
            part = result[(c - first) * span : (c - first + 1) * span]
            for k in range(part.shape[1] // 128):
                sbuf[c, begin + k, pl.ds(y, span, stride=ny), :] = part[:, k * 128 : (k + 1) * 128]

    def first_x(t):
        for y in range(0, ny, 2):
            load_v[t][y // 2].wait()
            for k in (y, y + 1):
                high, low = split(vbuf[t * per : (t + 1) * per, k].reshape(128, nx))
                vhi[k, t * 128 : (t + 1) * 128] = high
                vlo[k, t * 128 : (t + 1) * 128] = low
                transform_x(k, 0, FIRST, high, low, t)

    def north(c, t, start):
        slot = c % CYCLE * tiles + t if isinstance(c, int) else lax.rem(c, CYCLE) * tiles + t

        def copy(source, target, peer):
            return pltpu.make_async_remote_copy(
                src_ref=source,
                dst_ref=target,
                send_sem=ssem.at[0],
                recv_sem=rsem.at[slot],
                device_id={"north": peer, "deep": deep},
                device_id_type=MESH,
            )

        if not start:
            everything = rbuf.at[c, t, pl.ds(0, nn - 1)]
            return copy(everything, everything, me)
        for peer in farthest:
            copy(sbuf.at[c, t, pl.ds(pl.multiple_of(peer * piece, piece), piece)], rbuf.at[c, t, me], peer).start()
        rbuf[c, t, me] = sbuf[c, t, pl.ds(pl.multiple_of(me * piece, piece), piece), :]

    def vertical(c, t, start):
        slot = c % CYCLE * tiles + t if isinstance(c, int) else lax.rem(c, CYCLE) * tiles + t

        def copy(source, target, peer):
            return pltpu.make_async_remote_copy(
                src_ref=source,
                dst_ref=target,
                send_sem=dssem.at[0],
                recv_sem=drsem.at[slot],
                device_id={"north": me, "deep": peer},
                device_id_type=MESH,
            )

        if not start:
            everything = drecv.at[c, t, pl.ds(0, nd - 1)]
            return copy(everything, everything, deep)
        for peer in above:
            copy(dsend.at[c, t, peer], drecv.at[c, t, deep], peer).start()
        drecv[c, t, deep] = dsend[c, t, deep]

    def rest_x(start, stop):
        @pl.loop(start, stop)
        def _(y):
            transform_x(y, FIRST, chunks, vhi[y], vlo[y], 0)

    def stage_y(c, t):
        north(c, t, False).wait_recv()
        for j in range(rows):
            high, low = split(rbuf[c, t, :, pl.ds(j * ny, ny), :].reshape(full_y, 128))
            result = product(hy[0], hy[1], high, low)
            for d in range(nd):
                dsend[c, t, d, j] = result[d * share_y : (d + 1) * share_y]
        vertical(c, t, True)

    def weight_of(x):
        return 1.0 / (1.0 + (sym_x[me * share_x + x] + syz[...]))

    def stage_z(c):
        for t in range(tiles):
            vertical(c, t, False).wait_recv()
        for j in range(rows):
            x = c * rows + j
            old = transform_z([[drecv[c, t, d, j] for d in range(nd)] for t in range(tiles)], hy, nz)
            for a, values in enumerate(mixed_with(old, lambda a, b: coupling[a, b], weight_of(x))):
                out[a, x] = values

    loads[0].wait()
    first_x(0)
    for copy in loads[2:]:
        copy.start()
    pl.semaphore_wait(barrier, nn - 1 + nd - 1)
    north(0, 0, True)
    first_x(1)
    north(0, 1, True)
    loads[1].wait()
    rest_x(0, 2)
    north(1, 0, True)
    north(1, 1, True)
    rest_x(2, 4)
    for copy in loads[2:]:
        copy.wait()
    stage_y(0, 0)
    north(2, 0, True)
    rest_x(4, 6)
    stage_y(0, 1)
    north(2, 1, True)
    rest_x(6, 8)
    for c in range(FIRST, AHEAD):
        for t in range(tiles):
            north(c, t, True)

    lane = lax.broadcasted_iota(jnp.int32, (share_y, full_y), 1)
    row = lax.broadcasted_iota(jnp.int32, (share_y, full_y), 0)
    mine = jnp.where(lane == row + deep * share_y, sym_y[...], 0.0)
    syz[...] = jnp.sum(mine, axis=1, keepdims=True) + sym_z[...]

    def step(c, more, ready):
        stage_y(c, 0)
        if more:
            north(c + AHEAD - 1, 0, True)
        if ready:
            stage_z(c - LAG)
        stage_y(c, 1)
        if more:
            north(c + AHEAD - 1, 1, True)

    for first, last, more, ready in (
        (1, LAG, True, False),
        (LAG, chunks - AHEAD + 1, True, True),
        (chunks - AHEAD + 1, chunks, False, True),
    ):
        @pl.loop(first, last)
        def _(c):
            step(c, more, ready)

    @pl.loop(chunks - LAG, chunks - 1)
    def _(c):
        stage_z(c)

    table[...] = hy[...]
    weight[...] = weight_of(share_x - 1)
    for a in range(fields):
        for b in range(fields):
            mixing[pl.ds(a * fields + b, 1), :] = jnp.full((1, mixing.shape[1]), coupling[a, b], F32)
    for t in range(tiles):
        vertical(chunks - 1, t, False).wait_recv()
        for d in range(nd):
            tail[t, d] = drecv[chunks - 1, t, d, 0]

    for buffer, count, sent, received in ((rbuf, nn - 1, ssem, rsem), (drecv, nd - 1, dssem, drsem)):
        everything = buffer.at[:, :, pl.ds(0, count)]
        pltpu.make_async_remote_copy(
            src_ref=everything,
            dst_ref=everything,
            send_sem=sent.at[0],
            recv_sem=received.at[0],
            device_id={"north": me, "deep": deep},
            device_id_type=MESH,
        ).wait_send()


def on_device(nn, nd, velocity, coupling, symbol_x, symbol_y, symbol_z):
    fields, nx, ny, nz = velocity.shape
    share_x = nx // nn
    rows = share_x // CHUNKS
    full_y, full_z = ny * nn, nz * nd
    share_y = full_y // nd
    wide = fields * nz
    tiles = wide // 128
    order = np.arange(nx).reshape(nn, CHUNKS, rows).transpose(1, 0, 2).reshape(-1)
    table_x = jnp.asarray(two_parts(basis_table(nx)[order]))
    table_y = jnp.asarray(two_parts(basis_table(full_y)))
    dma = pltpu.SemaphoreType.DMA
    vector = pl.BlockSpec(memory_space=pltpu.VMEM)
    made = pl.pallas_call(
        functools.partial(kernel, nn, nd),
        out_shape=(
            jax.ShapeDtypeStruct((fields, share_x, share_y, full_z), F32),
            jax.ShapeDtypeStruct((tiles, nd, share_y, 128), F32),
            jax.ShapeDtypeStruct((2, full_y, full_y), BF16),
            jax.ShapeDtypeStruct((share_y, full_z), F32),
            jax.ShapeDtypeStruct((fields * fields, full_z), F32),
        ),
        in_specs=[pl.BlockSpec(memory_space=pltpu.MemorySpace.HBM)] * 7,
        out_specs=(vector,) * 5,
        scratch_shapes=[
            pltpu.VMEM((fields, ny, nz, nx), F32),
            pltpu.VMEM((ny, wide, nx), BF16),
            pltpu.VMEM((ny, wide, nx), BF16),
            pltpu.VMEM((2, nx, nx), BF16),
            pltpu.VMEM((2, full_y, full_y), BF16),
            pltpu.VMEM((CHUNKS, tiles, nn * rows * ny, 128), F32),
            pltpu.VMEM((CHUNKS, tiles, nn, rows * ny, 128), F32),
            pltpu.VMEM((CHUNKS, tiles, nd, rows, share_y, 128), F32),
            pltpu.VMEM((CHUNKS, tiles, nd, rows, share_y, 128), F32),
            pltpu.VMEM((share_y, full_z), F32),
            pltpu.SMEM((fields, fields), F32),
            pltpu.SMEM((nx,), F32),
            pltpu.VMEM((1, full_y), F32),
            pltpu.VMEM((1, full_z), F32),
            dma((tiles, ny // 2)), dma((7,)),
            dma((1,)), dma((CYCLE * tiles,)), dma((1,)), dma((CYCLE * tiles,)),
        ],
        compiler_params=pltpu.CompilerParams(
            collective_id=0, has_side_effects=True, vmem_limit_bytes=32 << 20
        ),
    )(*(
        pltpu.with_memory_space_constraint(array, pltpu.MemorySpace.HBM)
        for array in (
            jnp.transpose(velocity, (0, 2, 3, 1)), table_x, table_y, coupling, symbol_x,
            symbol_y.reshape(1, full_y), symbol_z.reshape(1, full_z),
        )
    ))

    return pl.pallas_call(
        functools.partial(finish, nz),
        out_shape=jax.ShapeDtypeStruct((fields, share_x, share_y, full_z), F32),
        in_specs=[vector] * 5,
        out_specs=pl.BlockSpec(memory_space=pl.ANY),
        scratch_shapes=[pltpu.VMEM((fields, share_y, full_z), F32), dma((2 * fields,))],
        compiler_params=pltpu.CompilerParams(vmem_limit_bytes=8 << 20),
    )(*made)


def solution(mesh):
    placed = (P(None, None, "north", "deep"), P(), P(), P(), P())
    return jax.shard_map(
        functools.partial(on_device, mesh.shape["north"], mesh.shape["deep"]),
        mesh=mesh,
        in_specs=placed,
        out_specs=P(None, "north", "deep", None),
        check_vma=False,
    )
```

```python
import functools

import jax
import jax.numpy as jnp
import numpy as np
from jax import lax
from jax.experimental import pallas as pl
from jax.experimental.pallas import tpu as pltpu
from jax.sharding import PartitionSpec as P

MESH = pl.DeviceIdType.MESH
F32, BF16 = jnp.float32, jnp.bfloat16
CHUNKS = 16
FIRST = 3
LAG = 3
AHEAD = 4
CYCLE = 8


def basis_table(count):
    rank = np.arange(1, count + 1)
    turns = (rank[:, None] * rank[None, :]) % (2 * count + 2)
    return np.sin(np.pi * turns / (count + 1)) * np.sqrt(2.0 / (count + 1))


def two_parts(table):
    high = table.astype(BF16)
    low = (table - high.astype(np.float64)).astype(BF16)
    return np.stack([high, low])


def split(values):
    high = values.astype(BF16)
    return high, (values - high.astype(F32)).astype(BF16)


def dot(a, b, transposed=False):
    dims = (((1,), (1 if transposed else 0,)), ((), ()))
    return lax.dot_general(a, b, dims, preferred_element_type=F32)


def product(a_high, a_low, b_high, b_low, transposed=False):
    count = a_high.shape[0]
    both = dot(jnp.concatenate([a_high, a_low], axis=0), b_high, transposed)
    return both[:count] + (both[count:] + dot(a_high, b_low, transposed))


def transform_z(pieces, table, nz):
    lower = lax.broadcasted_iota(jnp.int32, pieces[0][0].shape, 1) < nz
    lines = []
    for parts in pieces:
        turned = [pltpu.roll(p, nz, 1) for p in parts]
        pairs = range(0, len(parts), 2)
        even = [jnp.where(lower, parts[d], turned[d + 1]) for d in pairs]
        odd = [jnp.where(lower, turned[d], parts[d + 1]) for d in pairs]
        lines.append(jnp.concatenate(even, axis=1))
        lines.append(jnp.concatenate(odd, axis=1))
    high, low = split(jnp.concatenate(lines, axis=0))
    result = product(high, low, table[0], table[1])
    share = pieces[0][0].shape[0]
    return [result[f * share : (f + 1) * share] for f in range(len(lines))]


def mixed_with(old, coupling, weight):
    rest = 1.0 - weight
    for a in range(len(old)):
        mixed = coupling(a, 0) * old[0]
        for b in range(1, len(old)):
            mixed = mixed + coupling(a, b) * old[b]
        yield weight * old[a] + rest * mixed


def finish(nz, most, last, table, weight, coupling, result, final, sem):
    fields, share_x = most.shape[:2]
    copies = [
        pltpu.make_async_copy(most.at[f, pl.ds(0, share_x - 1)], result.at[f, pl.ds(0, share_x - 1)], sem.at[f])
        for f in range(fields)
    ]
    for copy in copies:
        copy.start()
    tiles, nd = last.shape[:2]
    old = transform_z([[last[t, d] for d in range(nd)] for t in range(tiles)], table, nz)

    def factor(a, b):
        return coupling[pl.ds(a * fields + b, 1), :]

    for a, values in enumerate(mixed_with(old, factor, weight[...])):
        final[a] = values
    copies.append(pltpu.make_async_copy(final, result.at[:, share_x - 1], sem.at[fields]))
    copies[-1].start()
    for copy in copies:
        copy.wait()


def kernel(
    nn, nd, v_hbm, hx_hbm, hy_hbm, coupling_hbm, sym_x_hbm, sym_y_hbm, sym_z_hbm, out, tail, table, weight, mixing,
    vbuf, vhi, vlo, hx, hy, sbuf, rbuf, dsend, drecv, syz, coupling, sym_x, sym_y, sym_z,
    vsem, hsem, ssem, rsem, dssem, drsem,
):
    fields, ny, nz, nx = v_hbm.shape
    chunks = sbuf.shape[0]
    share_x = nx // nn
    rows = share_x // chunks
    wide = fields * nz
    tiles = wide // 128
    full_y = nn * ny
    share_y = full_y // nd
    piece = rows * ny
    me, deep = lax.axis_index("north"), lax.axis_index("deep")

    soon = FIRST * nn * rows
    loads = [
        pltpu.make_async_copy(a, b, hsem.at[k])
        for k, (a, b) in enumerate((
            (hx_hbm.at[:, pl.ds(0, soon)], hx.at[:, pl.ds(0, soon)]),
            (hx_hbm.at[:, pl.ds(soon, nx - soon)], hx.at[:, pl.ds(soon, nx - soon)]), (hy_hbm, hy), (coupling_hbm, coupling), (sym_x_hbm, sym_x),
            (sym_y_hbm, sym_y), (sym_z_hbm, sym_z),
        ))
    ]
    per = fields // tiles
    load_v = [
        [
            pltpu.make_async_copy(
                v_hbm.at[pl.ds(t * per, per), pl.ds(y, 4)], vbuf.at[pl.ds(t * per, per), pl.ds(y, 4)], vsem.at[t, y // 4]
            )
            for y in range(0, ny, 4)
        ]
        for t in range(tiles)
    ]
    loads[0].start()
    for copy in load_v[0]:
        copy.start()

    along_y = [lax.rem(me // 8 + i, 4) * 8 for i in range(4)]
    along_x = [lax.rem(me // 2 + i, 4) * 2 for i in range(4)]
    cores = [lax.rem(me + i, 2) for i in range(2)]
    steps = [(a, b, c) for a in range(4) for b in range(4) for c in range(2)][1:]
    others = [along_y[a] + along_x[b] + cores[c] for a, b, c in steps]
    hops = [min(a, 4 - a) + min(b, 4 - b) for a, b, c in steps]
    farthest = [others[k] for k in sorted(range(len(steps)), key=lambda k: -hops[k])]
    above = [k + lax.div(k + nd - deep, nd) for k in range(nd - 1)]

    barrier = pltpu.get_barrier_semaphore()
    for peer in farthest:
        pl.semaphore_signal(
            barrier, inc=1, device_id={"north": peer, "deep": deep}, device_id_type=MESH
        )
    for peer in above:
        pl.semaphore_signal(
            barrier, inc=1, device_id={"north": me, "deep": peer}, device_id_type=MESH
        )

    for copy in load_v[1] + loads[1:2]:
        copy.start()

    def transform_x(y, first, last, high, low, begin):
        span = nn * rows
        pick = pl.ds(first * span, (last - first) * span)
        result = product(hx[0, pick, :], hx[1, pick, :], high, low, transposed=True)
        for c in range(first, last):
            part = result[(c - first) * span : (c - first + 1) * span]
            for k in range(part.shape[1] // 128):
                sbuf[c, begin + k, pl.ds(y, span, stride=ny), :] = part[:, k * 128 : (k + 1) * 128]

    def first_x(t):
        for y in range(0, ny, 4):
            load_v[t][y // 4].wait()
            for k in range(y, y + 4):
                high, low = split(vbuf[t * per : (t + 1) * per, k].reshape(128, nx))
                vhi[k, t * 128 : (t + 1) * 128] = high
                vlo[k, t * 128 : (t + 1) * 128] = low
                transform_x(k, 0, FIRST, high, low, t)

    def north(c, t, start):
        slot = c % CYCLE * tiles + t if isinstance(c, int) else lax.rem(c, CYCLE) * tiles + t

        def copy(source, target, peer):
            return pltpu.make_async_remote_copy(
                src_ref=source,
                dst_ref=target,
                send_sem=ssem.at[0],
                recv_sem=rsem.at[slot],
                device_id={"north": peer, "deep": deep},
                device_id_type=MESH,
            )

        if not start:
            everything = rbuf.at[c, t, pl.ds(0, nn - 1)]
            return copy(everything, everything, me)
        for peer in farthest:
            copy(sbuf.at[c, t, pl.ds(pl.multiple_of(peer * piece, piece), piece)], rbuf.at[c, t, me], peer).start()
        rbuf[c, t, me] = sbuf[c, t, pl.ds(pl.multiple_of(me * piece, piece), piece), :]

    def vertical(c, t, start):
        slot = c % CYCLE * tiles + t if isinstance(c, int) else lax.rem(c, CYCLE) * tiles + t

        def copy(source, target, peer):
            return pltpu.make_async_remote_copy(
                src_ref=source,
                dst_ref=target,
                send_sem=dssem.at[0],
                recv_sem=drsem.at[slot],
                device_id={"north": me, "deep": peer},
                device_id_type=MESH,
            )

        if not start:
            everything = drecv.at[c, t, pl.ds(0, nd - 1)]
            return copy(everything, everything, deep)
        for peer in above:
            copy(dsend.at[c, t, peer], drecv.at[c, t, deep], peer).start()
        drecv[c, t, deep] = dsend[c, t, deep]

    def rest_x(start, stop):
        @pl.loop(start, stop)
        def _(y):
            transform_x(y, FIRST, chunks, vhi[y], vlo[y], 0)

    def stage_y(c, t):
        north(c, t, False).wait_recv()
        for j in range(rows):
            high, low = split(rbuf[c, t, :, pl.ds(j * ny, ny), :].reshape(full_y, 128))
            result = product(hy[0], hy[1], high, low)
            for d in range(nd):
                dsend[c, t, d, j] = result[d * share_y : (d + 1) * share_y]
        vertical(c, t, True)

    def weight_of(x):
        return 1.0 / (1.0 + (sym_x[me * share_x + x] + syz[...]))

    def stage_z(c):
        for t in range(tiles):
            vertical(c, t, False).wait_recv()
        for j in range(rows):
            x = c * rows + j
            old = transform_z([[drecv[c, t, d, j] for d in range(nd)] for t in range(tiles)], hy, nz)
            for a, values in enumerate(mixed_with(old, lambda a, b: coupling[a, b], weight_of(x))):
                out[a, x] = values

    loads[0].wait()
    first_x(0)
    for copy in loads[2:]:
        copy.start()
    pl.semaphore_wait(barrier, nn - 1 + nd - 1)
    north(0, 0, True)
    first_x(1)
    north(0, 1, True)
    loads[1].wait()
    rest_x(0, 2)
    north(1, 0, True)
    north(1, 1, True)
    rest_x(2, 4)
    for copy in loads[2:]:
        copy.wait()
    stage_y(0, 0)
    north(2, 0, True)
    rest_x(4, 6)
    stage_y(0, 1)
    north(2, 1, True)
    rest_x(6, 8)
    for c in range(FIRST, AHEAD):
        for t in range(tiles):
            north(c, t, True)

    lane = lax.broadcasted_iota(jnp.int32, (share_y, full_y), 1)
    row = lax.broadcasted_iota(jnp.int32, (share_y, full_y), 0)
    mine = jnp.where(lane == row + deep * share_y, sym_y[...], 0.0)
    syz[...] = jnp.sum(mine, axis=1, keepdims=True) + sym_z[...]

    def step(c, more, ready):
        stage_y(c, 0)
        if more:
            north(c + AHEAD - 1, 0, True)
        if ready:
            stage_z(c - LAG)
        stage_y(c, 1)
        if more:
            north(c + AHEAD - 1, 1, True)

    for first, last, more, ready in (
        (1, LAG, True, False),
        (LAG, chunks - AHEAD + 1, True, True),
        (chunks - AHEAD + 1, chunks, False, True),
    ):
        @pl.loop(first, last)
        def _(c):
            step(c, more, ready)

    @pl.loop(chunks - LAG, chunks - 1)
    def _(c):
        stage_z(c)

    table[...] = hy[...]
    weight[...] = weight_of(share_x - 1)
    for a in range(fields):
        for b in range(fields):
            mixing[pl.ds(a * fields + b, 1), :] = jnp.full((1, mixing.shape[1]), coupling[a, b], F32)
    for t in range(tiles):
        vertical(chunks - 1, t, False).wait_recv()
        for d in range(nd):
            tail[t, d] = drecv[chunks - 1, t, d, 0]

    for buffer, count, sent, received in ((rbuf, nn - 1, ssem, rsem), (drecv, nd - 1, dssem, drsem)):
        everything = buffer.at[:, :, pl.ds(0, count)]
        pltpu.make_async_remote_copy(
            src_ref=everything,
            dst_ref=everything,
            send_sem=sent.at[0],
            recv_sem=received.at[0],
            device_id={"north": me, "deep": deep},
            device_id_type=MESH,
        ).wait_send()


def on_device(nn, nd, velocity, coupling, symbol_x, symbol_y, symbol_z):
    fields, nx, ny, nz = velocity.shape
    share_x = nx // nn
    rows = share_x // CHUNKS
    full_y, full_z = ny * nn, nz * nd
    share_y = full_y // nd
    wide = fields * nz
    tiles = wide // 128
    order = np.arange(nx).reshape(nn, CHUNKS, rows).transpose(1, 0, 2).reshape(-1)
    table_x = jnp.asarray(two_parts(basis_table(nx)[order]))
    table_y = jnp.asarray(two_parts(basis_table(full_y)))
    dma = pltpu.SemaphoreType.DMA
    vector = pl.BlockSpec(memory_space=pltpu.VMEM)
    made = pl.pallas_call(
        functools.partial(kernel, nn, nd),
        out_shape=(
            jax.ShapeDtypeStruct((fields, share_x, share_y, full_z), F32),
            jax.ShapeDtypeStruct((tiles, nd, share_y, 128), F32),
            jax.ShapeDtypeStruct((2, full_y, full_y), BF16),
            jax.ShapeDtypeStruct((share_y, full_z), F32),
            jax.ShapeDtypeStruct((fields * fields, full_z), F32),
        ),
        in_specs=[pl.BlockSpec(memory_space=pltpu.MemorySpace.HBM)] * 7,
        out_specs=(vector,) * 5,
        scratch_shapes=[
            pltpu.VMEM((fields, ny, nz, nx), F32),
            pltpu.VMEM((ny, wide, nx), BF16),
            pltpu.VMEM((ny, wide, nx), BF16),
            pltpu.VMEM((2, nx, nx), BF16),
            pltpu.VMEM((2, full_y, full_y), BF16),
            pltpu.VMEM((CHUNKS, tiles, nn * rows * ny, 128), F32),
            pltpu.VMEM((CHUNKS, tiles, nn, rows * ny, 128), F32),
            pltpu.VMEM((CHUNKS, tiles, nd, rows, share_y, 128), F32),
            pltpu.VMEM((CHUNKS, tiles, nd, rows, share_y, 128), F32),
            pltpu.VMEM((share_y, full_z), F32),
            pltpu.SMEM((fields, fields), F32),
            pltpu.SMEM((nx,), F32),
            pltpu.VMEM((1, full_y), F32),
            pltpu.VMEM((1, full_z), F32),
            dma((tiles, ny // 4)), dma((7,)),
            dma((1,)), dma((CYCLE * tiles,)), dma((1,)), dma((CYCLE * tiles,)),
        ],
        compiler_params=pltpu.CompilerParams(
            collective_id=0, has_side_effects=True, vmem_limit_bytes=32 << 20
        ),
    )(*(
        pltpu.with_memory_space_constraint(array, pltpu.MemorySpace.HBM)
        for array in (
            jnp.transpose(velocity, (0, 2, 3, 1)), table_x, table_y, coupling, symbol_x,
            symbol_y.reshape(1, full_y), symbol_z.reshape(1, full_z),
        )
    ))

    return pl.pallas_call(
        functools.partial(finish, nz),
        out_shape=jax.ShapeDtypeStruct((fields, share_x, share_y, full_z), F32),
        in_specs=[vector] * 5,
        out_specs=pl.BlockSpec(memory_space=pl.ANY),
        scratch_shapes=[pltpu.VMEM((fields, share_y, full_z), F32), dma((fields + 1,))],
        compiler_params=pltpu.CompilerParams(vmem_limit_bytes=8 << 20),
    )(*made)


def solution(mesh):
    placed = (P(None, None, "north", "deep"), P(), P(), P(), P())
    return jax.shard_map(
        functools.partial(on_device, mesh.shape["north"], mesh.shape["deep"]),
        mesh=mesh,
        in_specs=placed,
        out_specs=P(None, "north", "deep", None),
        check_vma=False,
    )
```
